32 devices in a mesh: row: 8 (over z, x), col: 4 (over y, core).
Axes of the slice: x: 2, y: 2, z: 4, core: 2. Of those that a mesh axis runs over, the one named last changes fastest.
Arguments:
- tile_values: bfloat16 [192, 512, 128], P('row', 'col'), may hold values from -0.0546875 to 0.0546875
- tile_counts: int32 [96, 4], P('row', 'col'), may hold values from 0 to 2, as said below
- tile_cols: int32 [192, 4], P('row', 'col'), may hold values from 0 to 1, as said below
- panels: bfloat16 [12288, 4096], P('row', 'col'), may hold values from -6 to 6
Outputs:
- product: bfloat16 [1024, 4096], P('col', 'row')
The draws below stay inside these ranges and needn't reach their ends.
Inputs may be any that keep to these rules, and one draw needn't show every extreme that they name: `tile_counts`: within each device the filled slots follow block row order; a device holds at most 24 tiles and some device holds exactly 24 in every draw. `tile_cols`: within one block row of a device the filled slots' columns rise strictly; entries of unfilled slots carry no meaning.
All inputs are finite; a program needn't handle non-finite values.
Results may differ from the reference program's by a relative error of at most 0.001.
Values may be sent and summed in bfloat16 or wider, within the bound.
No kernel may reach another device: no remote copies, remote signals or barrier semaphores. Data moves between devices by JAX's collectives and lax.ppermute only.
A program may use at most 64 MiB of HBM per device.

```python
import jax
import jax.numpy as jnp
from jax import lax

TILE = 128
NB = 4096
BR_DEV = 12
BC_DEV = 2
CAP = 24
ROWS = 12288
COLS = 1024
N_ROW = 8
N_COL = 4


def tile_pattern(key):
    base = jax.random.fold_in(key, 7)
    key_levels = jax.random.fold_in(base, 1)
    key_rolled = jax.random.fold_in(base, 2)
    key_chosen = jax.random.fold_in(base, 3)
    levels = jax.random.randint(key_levels, (N_ROW, N_COL, BR_DEV, 1), 0, 5)
    chosen = jax.random.randint(key_chosen, (), 0, N_ROW * N_COL)
    device_ids = jnp.arange(N_ROW, dtype=jnp.int32)[:, None] * N_COL + jnp.arange(N_COL, dtype=jnp.int32)[None, :]
    levels = jnp.where((device_ids == chosen)[:, :, None, None], 4, levels)
    rolled = jax.random.randint(key_rolled, (N_ROW, N_COL, BR_DEV, BC_DEV), 0, 4)
    present = (rolled < levels).astype(jnp.int32)
    counts = jnp.sum(present, axis=-1).astype(jnp.int32)
    row_start = (jnp.cumsum(counts, axis=-1) - counts).astype(jnp.int32)
    within = (jnp.cumsum(present, axis=-1) - present).astype(jnp.int32)
    slot_index = jnp.where(present == 1, row_start[..., None] + within, CAP).astype(jnp.int32)
    col_index = jnp.broadcast_to(jnp.arange(BC_DEV, dtype=jnp.int32), present.shape)

    def place_row(slots, values):
        return jnp.zeros((CAP,), jnp.int32).at[slots].set(values, mode='drop')
    columns = jax.vmap(place_row)(slot_index.reshape(N_ROW * N_COL, BR_DEV * BC_DEV), col_index.reshape(N_ROW * N_COL, BR_DEV * BC_DEV))
    return (counts, columns.reshape(N_ROW, N_COL, CAP))


def draw_tile_counts(key, part):
    counts, columns = tile_pattern(key)
    return jnp.transpose(counts, (0, 2, 1)).reshape(N_ROW * BR_DEV, N_COL)


def draw_tile_cols(key, part):
    counts, columns = tile_pattern(key)
    return jnp.transpose(columns, (0, 2, 1)).reshape(N_ROW * CAP, N_COL)


def strengthened(array, stream_key, source, target, blocks, factor):
    owner, partner = [(jnp.arange(array.shape[dim]) // (array.shape[dim] // blocks)).reshape([-1 if axis == dim else 1 for axis in range(array.ndim)]) for dim in (source, target)]
    chosen = jax.random.permutation(stream_key, blocks)[partner]
    strong = (owner == chosen) | (owner == (partner + blocks // 2) % blocks)
    return jnp.where(strong, factor * array, array)


def block_levels(stream_key, dims, split, smallest, top_value):
    factor_of, own = 1.0, jax.random.fold_in(stream_key, 6)
    for axis_at, blocks in split:
        steps = jnp.exp(jax.random.uniform(jax.random.fold_in(own, axis_at), (blocks,), jnp.float32, smallest / len(split), top_value / len(split)))
        factor_of = factor_of * jnp.repeat(steps, dims[axis_at] // blocks).reshape([-1 if axis == axis_at else 1 for axis in range(len(dims))])
    return factor_of


def centred(stream_key, dims, width, reach, cuts=(), kind=jnp.bfloat16):
    entries = width * jax.random.normal(stream_key, dims, jnp.float32)
    if cuts:
        entries = entries * block_levels(stream_key, dims, cuts, -0.22, 0.18)
    return jnp.clip(entries, -reach, reach).astype(kind)


def noise_with(key, shape, width, reach, shards, heavy, held_as=jnp.bfloat16):
    drawn = width * jax.random.normal(key, shape, jnp.float32)
    if shards:
        drawn = drawn * block_levels(key, shape, shards, -0.22, 0.18)
    return jnp.clip(strengthened(drawn, jax.random.fold_in(key, 3), *heavy), -reach, reach).astype(held_as)


def setup_inputs(seed: int = 0) -> dict:
    key_of = jax.random.split(jax.random.key(seed), 5)
    return {
        "tile_values": centred(key_of[0], (N_ROW * CAP, N_COL * TILE, TILE), (TILE * BR_DEV * N_ROW) ** -0.5, 0.0546875, ((0, 8), (1, 4))),
        "tile_counts": draw_tile_counts(jax.random.fold_in(key_of[4], 71), 0),
        "tile_cols": draw_tile_cols(jax.random.fold_in(key_of[4], 71), 0),
        "panels": noise_with(key_of[3], (ROWS, NB), 1.0, 6.0, ((0, 8), (1, 4)), (0, 1, 8, 2.0)),
    }


def reference(tile_values, tile_counts, tile_cols, panels):
    def add_group(row_dev, totals):
        row_dev = jnp.asarray(row_dev).astype(jnp.int32)
        tile_slab = lax.dynamic_slice_in_dim(tile_values, row_dev * CAP, CAP, 0)
        tile_slab = tile_slab.astype(jnp.float32).reshape(CAP, N_COL, TILE, TILE)
        counts = lax.dynamic_slice_in_dim(tile_counts, row_dev * BR_DEV, BR_DEV, 0).astype(jnp.int32)
        columns = lax.dynamic_slice_in_dim(tile_cols, row_dev * CAP, CAP, 0).astype(jnp.int32)
        row_start = (jnp.cumsum(counts, axis=0) - counts).astype(jnp.int32)
        slot_ids = jnp.arange(CAP, dtype=jnp.int32)[:, None, None]
        row_mask = ((slot_ids >= row_start[None]) & (slot_ids < (row_start + counts)[None])).astype(jnp.float32)
        col_mask = (columns[:, None, :] == jnp.arange(BC_DEV, dtype=jnp.int32)[None, :, None]).astype(jnp.float32)
        dense_rows = jnp.einsum("sic,sjc,scab->iacjb", row_mask, col_mask, tile_slab)
        dense_rows = dense_rows.reshape(BR_DEV * TILE, N_COL * BC_DEV * TILE).astype(jnp.bfloat16)
        panel_rows = lax.dynamic_slice_in_dim(panels, row_dev * BR_DEV * TILE, BR_DEV * TILE, 0)
        return totals + lax.dot_general(dense_rows, panel_rows, (((0,), (0,)), ((), ())), preferred_element_type=jnp.float32)

    totals = lax.fori_loop(0, N_ROW, add_group, jnp.zeros((COLS, NB), jnp.float32))
    return totals.astype(jnp.bfloat16)
```

```python
import jax
import jax.numpy as jnp
from jax import lax
from jax.sharding import PartitionSpec as P


def dense_block(tile_values, tile_counts, tile_cols, wide):
    slots, edge, _ = tile_values.shape
    tall = tile_counts.shape[0]
    counts = tile_counts[:, 0]
    row_start = jnp.cumsum(counts) - counts
    slot_ids = jnp.arange(slots, dtype=jnp.int32)[:, None]
    row_mask = (slot_ids >= row_start[None, :]) & (slot_ids < (row_start + counts)[None, :])
    col_mask = tile_cols == jnp.arange(wide, dtype=jnp.int32)[None, :]
    selector = (row_mask[:, :, None] & col_mask[:, None, :]).astype(jnp.bfloat16)
    dense = jnp.einsum("sij,sab->iajb", selector, tile_values, preferred_element_type=jnp.float32)
    return dense.astype(jnp.bfloat16).reshape(tall * edge, wide * edge)


def product(a, b):
    return lax.dot_general(a, b, (((0,), (0,)), ((), ())), preferred_element_type=jnp.float32)


def solution(mesh):
    rows, cols = mesh.shape["row"], mesh.shape["col"]
    spread = rows // cols
    assert spread == 2 and cols & (cols - 1) == 0

    def permute(value, move):
        pairs = [
            (r * cols + c, to[0] * cols + to[1])
            for r in range(rows)
            for c in range(cols)
            if (to := move(r, c)) is not None
        ]
        return lax.ppermute(value, ("row", "col"), pairs)

    def per_device(tile_values, tile_counts, tile_cols, panels):
        depth, width = panels.shape
        edge = tile_values.shape[2]
        wide = (depth // edge * 2 + tile_values.shape[0] - 1) // tile_values.shape[0]
        wide = tile_values.shape[0] // tile_counts.shape[0]
        dense = {0: dense_block(tile_values, tile_counts, tile_cols, wide)}
        bit = cols // 2
        while bit:
            for m in list(dense):
                dense[m ^ bit] = permute(dense[m], lambda r, c: (r, c ^ bit))
            bit //= 2

        half = width // spread
        side = lax.axis_index("row") % spread
        b_keep = lax.dynamic_slice_in_dim(panels, side * half, half, 1)
        b_send = lax.dynamic_slice_in_dim(panels, (1 - side) * half, half, 1)

        out = 0
        for m in range(cols):
            sent = product(dense[m], b_send)
            kept = product(dense[m], b_keep)
            total = kept + permute(sent, lambda r, c: (r ^ 1, c))
            bit = 1
            while bit < cols:
                def fold(r, c):
                    q = r // spread
                    low = bit - 1
                    if (q ^ c) & low or not (q ^ c) & bit:
                        return None
                    return (r ^ (bit * spread), c)

                total = total + permute(total, fold)
                bit *= 2
            final = total.astype(jnp.bfloat16)
            mine = lax.axis_index("row") // spread == lax.axis_index("col")
            if m:
                got = permute(final, lambda r, c: (r, c ^ m) if r // spread == c else None)
                out = out + got
            else:
                out = jnp.where(mine, final, jnp.zeros_like(final))
        return out

    return jax.shard_map(
        per_device,
        mesh=mesh,
        in_specs=(P("row", "col", None), P("row", "col"), P("row", "col"), P("row", "col")),
        out_specs=P("col", "row"),
        check_vma=False,
    )
```

```python
import jax
import jax.numpy as jnp
from jax import lax
from jax.sharding import PartitionSpec as P


def dense_block(tile_values, tile_counts, tile_cols, wide):
    slots, edge, _ = tile_values.shape
    tall = tile_counts.shape[0]
    counts = tile_counts[:, 0]
    row_start = jnp.cumsum(counts) - counts
    slot_ids = jnp.arange(slots, dtype=jnp.int32)[:, None]
    row_mask = (slot_ids >= row_start[None, :]) & (slot_ids < (row_start + counts)[None, :])
    col_mask = tile_cols == jnp.arange(wide, dtype=jnp.int32)[None, :]
    selector = (row_mask[:, :, None] & col_mask[:, None, :]).astype(jnp.bfloat16)
    dense = jnp.einsum("sij,sab->iajb", selector, tile_values, preferred_element_type=jnp.float32)
    return dense.astype(jnp.bfloat16).reshape(tall * edge, wide * edge)


def product(a, b):
    return lax.dot_general(a, b, (((0,), (0,)), ((), ())), preferred_element_type=jnp.float32)


def solution(mesh):
    rows, cols = mesh.shape["row"], mesh.shape["col"]
    spread = rows // cols
    assert spread == 2 and rows & (rows - 1) == 0

    def permute(value, move):
        pairs = [
            (r * cols + c, to[0] * cols + to[1])
            for r in range(rows)
            for c in range(cols)
            if (to := move(r, c)) is not None
        ]
        return lax.ppermute(value, ("row", "col"), pairs)

    def per_device(tile_values, tile_counts, tile_cols, panels):
        depth, width = panels.shape
        half = width // spread
        wide = tile_values.shape[0] // tile_counts.shape[0]
        r, c = lax.axis_index("row"), lax.axis_index("col")
        side = r % spread
        other = permute(panels, lambda r, c: (r, c ^ 1))
        own_stays = (r // spread) % 2 == c % 2

        dense = {0: dense_block(tile_values, tile_counts, tile_cols, wide)}
        bit = cols // 2
        while bit > 1:
            for m in list(dense):
                dense[m ^ bit] = permute(dense[m], lambda r, c: (r, c ^ bit))
            bit //= 2

        def columns(array, index):
            return lax.dynamic_slice_in_dim(array, index * half, half, 1)

        out = None
        for m in dense:
            sent = jnp.concatenate(
                [product(dense[m], columns(panels, 1 - side)), product(dense[m], columns(other, 1 - side))], 0
            )
            kept = jnp.concatenate(
                [product(dense[m], columns(panels, side)), product(dense[m], columns(other, side))], 0
            )
            total = kept + permute(sent, lambda r, c: (r ^ 1, c))
            mine, partners = jnp.split(total, 2, 0)
            keep = jnp.where(own_stays, mine, partners)
            send = jnp.where(own_stays, partners, mine)
            total = keep + permute(send, lambda r, c: (r ^ spread, c))
            bit = 2
            while bit < cols:

                def fold(r, c):
                    apart = (r // spread) ^ c
                    if not apart & bit or apart & (bit - 2):
                        return None
                    return (r ^ (bit * spread), c)

                total = total + permute(total, fold)
                bit *= 2
            final = total.astype(jnp.bfloat16)
            rooted = (r // spread) // 2 == c // 2
            if m:
                out = out + permute(final, lambda r, c: (r, c ^ m) if r // spread // 2 == c // 2 else None)
            else:
                out = jnp.where(rooted, final, jnp.zeros_like(final))
        return out

    return jax.shard_map(
        per_device,
        mesh=mesh,
        in_specs=(P("row", "col", None), P("row", "col"), P("row", "col"), P("row", "col")),
        out_specs=P("col", "row"),
        check_vma=False,
    )
```

```python
import functools

import jax
import jax.numpy as jnp
from jax import lax
from jax.experimental import pallas as pl
from jax.experimental.pallas import tpu as pltpu
from jax.sharding import PartitionSpec as P


GROUPS = 2
SUB = 8
TOP = 32767.0
STEPS = 128.0
VMEM = pl.BlockSpec(memory_space=pltpu.VMEM)
SMEM = pl.BlockSpec(memory_space=pltpu.SMEM)


def encode(value, ref):
    height, width = value.shape
    part = height // GROUPS
    for g in range(GROUPS):
        rows = value[g * part : (g + 1) * part].reshape(part // SUB, SUB, width)
        largest = jnp.max(jnp.abs(rows), axis=0)
        code = jnp.ceil(jnp.log2(jnp.maximum(largest, 1e-30)) * STEPS)
        factor = TOP / jnp.exp2(code / STEPS)
        whole = jnp.clip(jnp.round(rows * factor[None]), -TOP, TOP).astype(jnp.int32)
        ref[g * part : (g + 1) * part] = whole.reshape(part, width).astype(jnp.int16)
        whole = code.astype(jnp.int32)
        code_rows = whole if g == 0 else jnp.concatenate([code_rows, whole], 0)
    ref[height : height + GROUPS * SUB] = code_rows.astype(jnp.int16)


def decode(coded, height):
    width = coded.shape[1]
    part = height // GROUPS
    codes = coded[height : height + GROUPS * SUB].astype(jnp.int32).astype(jnp.float32)
    pieces = []
    for g in range(GROUPS):
        scale = jnp.exp2(codes[g * SUB : (g + 1) * SUB] / STEPS) * (1.0 / TOP)
        rows = coded[g * part : (g + 1) * part].astype(jnp.int32).astype(jnp.float32)
        pieces.append((rows.reshape(part // SUB, SUB, width) * scale[None]).reshape(part, width))
    return jnp.concatenate(pieces, 0)


def build_kernel(counts, columns, tiles, *outs):
    tall, wide, slots = counts.shape[0], len(outs), tiles.shape[0]
    edge = tiles.shape[1]
    start = jnp.int32(0)
    for i in range(tall):
        count = counts[i, 0]
        for j, out in enumerate(outs):
            slot, found = jnp.int32(0), jnp.int32(0)
            for t in range(wide):
                at = jnp.minimum(start + t, slots - 1)
                hit = (t < count) & (columns[at, 0] == j)
                slot = jnp.where(hit, at, slot)
                found = jnp.where(hit, 1, found)
            tile = tiles[slot].astype(jnp.float32) * found.astype(jnp.float32)
            out[:, i * edge : (i + 1) * edge] = tile.T.astype(jnp.bfloat16)
        start = start + count


def build(tile_values, tile_counts, tile_cols):
    slots, edge, _ = tile_values.shape
    tall = tile_counts.shape[0]
    shape = jax.ShapeDtypeStruct((edge, tall * edge), jnp.bfloat16)
    return pl.pallas_call(
        build_kernel,
        out_shape=[shape] * (slots // tall),
        in_specs=[SMEM, SMEM, VMEM],
        out_specs=[VMEM] * (slots // tall),
        name="build",
    )(tile_counts, tile_cols, tile_values)


def product_kernel(place, *refs, count, coded):
    del place
    blocks, (own, other), out = refs[:count], refs[count : count + 2], refs[-1]
    a = jnp.concatenate([b[...] for b in blocks], 0) if count > 1 else blocks[0][...]
    value = jnp.concatenate(
        [jnp.dot(a, b[...], preferred_element_type=jnp.float32) for b in (own, other)], 0
    )
    if coded:
        encode(value, out)
    else:
        out[...] = value


def products(place, blocks, own, other, half, coded):
    edge, depth = blocks[0].shape
    height = 2 * edge * len(blocks)
    step = min(half, 256)
    per = half // step
    if coded:
        shape = jax.ShapeDtypeStruct((height + GROUPS * SUB, half), jnp.int16)
        columns = lambda n, s: (0, (1 - s[0]) * per + n)
    else:
        shape = jax.ShapeDtypeStruct((height, half), jnp.float32)
        columns = lambda n, s: (0, s[0] * per + n)
    return pl.pallas_call(
        functools.partial(product_kernel, count=len(blocks), coded=coded),
        out_shape=shape,
        grid_spec=pltpu.PrefetchScalarGridSpec(
            num_scalar_prefetch=1,
            grid=(per,),
            in_specs=[pl.BlockSpec((edge, depth), lambda n, s: (0, 0)) for _ in blocks]
            + [pl.BlockSpec((depth, step), columns)] * 2,
            out_specs=pl.BlockSpec((shape.shape[0], step), lambda n, s: (0, n)),
        ),
        name="leaving" if coded else "staying",
    )(place, *blocks, own, other)


def split_kernel(place, coded, kept, hold, send):
    height = kept.shape[0] // 2
    value = kept[...] + decode(coded[...], 2 * height)
    first, second = value[:height], value[height:]
    stays = place[1] == 0
    hold[...] = jnp.where(stays, first, second)
    encode(jnp.where(stays, second, first), send)


def split(place, coded, kept):
    height, half = kept.shape[0] // 2, kept.shape[1]
    return pl.pallas_call(
        split_kernel,
        out_shape=[
            jax.ShapeDtypeStruct((height, half), jnp.float32),
            jax.ShapeDtypeStruct((height + GROUPS * SUB, half), jnp.int16),
        ],
        in_specs=[SMEM, VMEM, VMEM],
        out_specs=[VMEM, VMEM],
        name="split",
    )(place, coded, kept)


def merge_kernel(coded, kept, hold, send):
    value = kept[...] + decode(coded[...], kept.shape[0])
    hold[...] = value
    encode(value, send)


def merge(coded, kept):
    height, half = kept.shape
    return pl.pallas_call(
        merge_kernel,
        out_shape=[
            jax.ShapeDtypeStruct((height, half), jnp.float32),
            jax.ShapeDtypeStruct((height + GROUPS * SUB, half), jnp.int16),
        ],
        in_specs=[VMEM, VMEM],
        out_specs=[VMEM, VMEM],
        name="merge",
    )(coded, kept)


def finish_kernel(coded, kept, out):
    out[...] = (kept[...] + decode(coded[...], kept.shape[0])).astype(jnp.bfloat16)


def finish(coded, kept):
    return pl.pallas_call(
        finish_kernel,
        out_shape=jax.ShapeDtypeStruct(kept.shape, jnp.bfloat16),
        in_specs=[VMEM, VMEM],
        out_specs=VMEM,
        name="finish",
    )(coded, kept)


def solution(mesh):
    rows, cols = mesh.shape["row"], mesh.shape["col"]
    spread = rows // cols
    assert spread == 2 and rows & (rows - 1) == 0 and cols >= 4

    def permute(value, move):
        pairs = [
            (r * cols + c, to[0] * cols + to[1])
            for r in range(rows)
            for c in range(cols)
            if (to := move(r, c)) is not None
        ]
        return lax.ppermute(value, ("row", "col"), pairs)

    def per_device(tile_values, tile_counts, tile_cols, panels):
        half = panels.shape[1] // spread
        r, c = lax.axis_index("row"), lax.axis_index("col")
        place = jnp.stack([r % spread, (r // spread + c) % 2]).astype(jnp.int32)
        other = permute(panels, lambda r, c: (r, c ^ 1))

        own = build(tile_values, tile_counts, tile_cols)
        dense = {0: own}
        bit = cols // 2
        while bit > 1:
            for m in list(dense):
                dense[m ^ bit] = [permute(block, lambda r, c: (r, c ^ bit)) for block in dense[m]]
            bit //= 2

        def reduced(blocks):
            sent = products(place, blocks, panels, other, half, True)
            kept = products(place, blocks, panels, other, half, False)
            hold, send = split(place, permute(sent, lambda r, c: (r ^ 1, c)), kept)
            got = permute(send, lambda r, c: (r ^ spread, c))
            bit = 2
            while bit < cols:

                def fold(r, c):
                    apart = (r // spread) ^ c
                    if not apart & bit or apart & (bit - 2):
                        return None
                    return (r ^ (bit * spread), c)

                hold, send = merge(got, hold)
                got = permute(send, fold)
                bit *= 2
            return finish(got, hold)

        def rooted(r, c):
            return (r // spread) // 2 == c // 2

        local = reduced(own)
        pieces = []
        for j in range(len(own)):
            piece = 0
            for m in dense:
                if m:
                    final = reduced([dense[m][j]])
                    piece = piece + permute(final, lambda r, c: (r, c ^ m) if rooted(r, c) else None)
            pieces.append(piece)
        return jnp.where(rooted(r, c), local, jnp.concatenate(pieces, 0))

    return jax.shard_map(
        per_device,
        mesh=mesh,
        in_specs=(P("row", "col", None), P("row", "col"), P("row", "col"), P("row", "col")),
        out_specs=P("col", "row"),
        check_vma=False,
    )
```

```python
import functools

import jax
import jax.numpy as jnp
from jax import lax
from jax.experimental import pallas as pl
from jax.experimental.pallas import tpu as pltpu
from jax.sharding import PartitionSpec as P


GROUPS = 2
SUB = 8
TOP = 32767.0
STEPS = 128.0
VMEM = pl.BlockSpec(memory_space=pltpu.VMEM)
SMEM = pl.BlockSpec(memory_space=pltpu.SMEM)
SMALL = pltpu.CompilerParams(vmem_limit_bytes=16 * 2**20)


def encode(value, ref, at=slice(None)):
    height, width = value.shape
    part = height // GROUPS
    for g in range(GROUPS):
        rows = value[g * part : (g + 1) * part].reshape(part // SUB, SUB, width)
        largest = jnp.max(jnp.abs(rows), axis=0)
        code = jnp.ceil(jnp.log2(jnp.maximum(largest, 1e-30)) * STEPS)
        factor = TOP / jnp.exp2(code / STEPS)
        whole = jnp.clip(jnp.round(rows * factor[None]), -TOP, TOP).astype(jnp.int32)
        ref[g * part : (g + 1) * part, at] = whole.reshape(part, width).astype(jnp.int16)
        whole = code.astype(jnp.int32)
        code_rows = whole if g == 0 else jnp.concatenate([code_rows, whole], 0)
    ref[height : height + GROUPS * SUB, at] = code_rows.astype(jnp.int16)


def decode(coded, height):
    width = coded.shape[1]
    part = height // GROUPS
    codes = coded[height : height + GROUPS * SUB].astype(jnp.int32).astype(jnp.float32)
    pieces = []
    for g in range(GROUPS):
        scale = jnp.exp2(codes[g * SUB : (g + 1) * SUB] / STEPS) * (1.0 / TOP)
        rows = coded[g * part : (g + 1) * part].astype(jnp.int32).astype(jnp.float32)
        pieces.append((rows.reshape(part // SUB, SUB, width) * scale[None]).reshape(part, width))
    return jnp.concatenate(pieces, 0)


def build_kernel(counts, columns, tiles, *outs):
    tall, wide, slots = counts.shape[0], len(outs), tiles.shape[0]
    edge = tiles.shape[1]
    start = jnp.int32(0)
    for i in range(tall):
        count = counts[i]
        for j, out in enumerate(outs):
            slot, found = jnp.int32(0), jnp.int32(0)
            for t in range(wide):
                at = jnp.minimum(start + t, slots - 1)
                hit = (t < count) & (columns[at] == j)
                slot = jnp.where(hit, at, slot)
                found = jnp.where(hit, 1, found)
            tile = tiles[slot].astype(jnp.float32) * found.astype(jnp.float32)
            out[:, i * edge : (i + 1) * edge] = tile.T.astype(jnp.bfloat16)
        start = start + count


def build(tile_values, tile_counts, tile_cols):
    slots, edge, _ = tile_values.shape
    tall = tile_counts.shape[0]
    shape = jax.ShapeDtypeStruct((edge, tall * edge), jnp.bfloat16)
    return pl.pallas_call(
        build_kernel,
        out_shape=[shape] * (slots // tall),
        in_specs=[SMEM, SMEM, VMEM],
        out_specs=[VMEM] * (slots // tall),
        compiler_params=SMALL,
        name="build",
    )(tile_counts[:, 0], tile_cols[:, 0], tile_values)


def product_kernel(place, *refs, count, coded):
    blocks, panels, out = refs[:count], refs[count : count + 2], refs[-1]
    a = jnp.concatenate([b[...] for b in blocks], 0) if count > 1 else blocks[0][...]
    half = out.shape[1]
    step = min(half, 256)
    start = (1 - place[0] if coded else place[0]) * half
    for n in range(0, half, step):
        at = pl.multiple_of(start + n, step)
        value = jnp.concatenate(
            [jnp.dot(a, b[:, pl.ds(at, step)], preferred_element_type=jnp.float32) for b in panels], 0
        )
        if coded:
            encode(value, out, slice(n, n + step))
        else:
            out[:, n : n + step] = value


def products(place, blocks, own, other, half, coded):
    height = 2 * blocks[0].shape[0] * len(blocks)
    if coded:
        shape = jax.ShapeDtypeStruct((height + GROUPS * SUB, half), jnp.int16)
    else:
        shape = jax.ShapeDtypeStruct((height, half), jnp.float32)
    return pl.pallas_call(
        functools.partial(product_kernel, count=len(blocks), coded=coded),
        out_shape=shape,
        in_specs=[SMEM] + [VMEM] * (len(blocks) + 2),
        out_specs=VMEM,
        compiler_params=SMALL,
        name="leaving" if coded else "staying",
    )(place, *blocks, own, other)


def split_kernel(place, coded, kept, hold, send):
    height = kept.shape[0] // 2
    value = kept[...] + decode(coded[...], 2 * height)
    first, second = value[:height], value[height:]
    stays = place[1] == 0
    hold[...] = jnp.where(stays, first, second)
    encode(jnp.where(stays, second, first), send)


def split(place, coded, kept):
    height, half = kept.shape[0] // 2, kept.shape[1]
    return pl.pallas_call(
        split_kernel,
        out_shape=[
            jax.ShapeDtypeStruct((height, half), jnp.float32),
            jax.ShapeDtypeStruct((height + GROUPS * SUB, half), jnp.int16),
        ],
        in_specs=[SMEM, VMEM, VMEM],
        out_specs=[VMEM, VMEM],
        compiler_params=SMALL,
        name="split",
    )(place, coded, kept)


def merge_kernel(coded, kept, hold, send):
    value = kept[...] + decode(coded[...], kept.shape[0])
    hold[...] = value
    encode(value, send)


def merge(coded, kept):
    height, half = kept.shape
    return pl.pallas_call(
        merge_kernel,
        out_shape=[
            jax.ShapeDtypeStruct((height, half), jnp.float32),
            jax.ShapeDtypeStruct((height + GROUPS * SUB, half), jnp.int16),
        ],
        in_specs=[VMEM, VMEM],
        out_specs=[VMEM, VMEM],
        compiler_params=SMALL,
        name="merge",
    )(coded, kept)


def finish_kernel(coded, kept, out):
    out[...] = (kept[...] + decode(coded[...], kept.shape[0])).astype(jnp.bfloat16)


def finish(coded, kept):
    return pl.pallas_call(
        finish_kernel,
        out_shape=jax.ShapeDtypeStruct(kept.shape, jnp.bfloat16),
        in_specs=[VMEM, VMEM],
        out_specs=VMEM,
        compiler_params=SMALL,
        name="finish",
    )(coded, kept)


def solution(mesh):
    rows, cols = mesh.shape["row"], mesh.shape["col"]
    spread = rows // cols
    assert spread == 2 and rows & (rows - 1) == 0 and cols >= 4

    def permute(value, move):
        pairs = [
            (r * cols + c, to[0] * cols + to[1])
            for r in range(rows)
            for c in range(cols)
            if (to := move(r, c)) is not None
        ]
        return lax.ppermute(value, ("row", "col"), pairs)

    def per_device(tile_values, tile_counts, tile_cols, panels):
        half = panels.shape[1] // spread
        r, c = lax.axis_index("row"), lax.axis_index("col")
        place = jnp.stack([r % spread, (r // spread + c) % 2]).astype(jnp.int32)
        other = permute(panels, lambda r, c: (r, c ^ 1))

        own = build(tile_values, tile_counts, tile_cols)
        dense = {0: own}
        bit = cols // 2
        while bit > 1:
            for m in list(dense):
                dense[m ^ bit] = [permute(block, lambda r, c: (r, c ^ bit)) for block in dense[m]]
            bit //= 2

        def reduced(blocks):
            sent = products(place, blocks, panels, other, half, True)
            kept = products(place, blocks, panels, other, half, False)
            hold, send = split(place, permute(sent, lambda r, c: (r ^ 1, c)), kept)
            got = permute(send, lambda r, c: (r ^ spread, c))
            bit = 2
            while bit < cols:

                def fold(r, c):
                    apart = (r // spread) ^ c
                    if not apart & bit or apart & (bit - 2):
                        return None
                    return (r ^ (bit * spread), c)

                hold, send = merge(got, hold)
                got = permute(send, fold)
                bit *= 2
            return finish(got, hold)

        def rooted(r, c):
            return (r // spread) // 2 == c // 2

        local = reduced(own)
        pieces = []
        for j in range(len(own)):
            piece = 0
            for m in dense:
                if m:
                    final = reduced([dense[m][j]])
                    piece = piece + permute(final, lambda r, c: (r, c ^ m) if rooted(r, c) else None)
            pieces.append(piece)
        return jnp.where(rooted(r, c), local, jnp.concatenate(pieces, 0))

    return jax.shard_map(
        per_device,
        mesh=mesh,
        in_specs=(P("row", "col", None), P("row", "col"), P("row", "col"), P("row", "col")),
        out_specs=P("col", "row"),
        check_vma=False,
    )
```

```python
import functools

import jax
import jax.numpy as jnp
from jax import lax
from jax.experimental import pallas as pl
from jax.experimental.pallas import tpu as pltpu
from jax.sharding import PartitionSpec as P


GROUPS = 2
SUB = 8
TOP = 32767.0
STEPS = 128.0
VMEM = pl.BlockSpec(memory_space=pltpu.VMEM)
SMEM = pl.BlockSpec(memory_space=pltpu.SMEM)
SMALL = pltpu.CompilerParams(vmem_limit_bytes=16 * 2**20)


def encode(value, ref, at=slice(None)):
    height, width = value.shape
    part = height // GROUPS
    for g in range(GROUPS):
        rows = value[g * part : (g + 1) * part].reshape(part // SUB, SUB, width)
        largest = jnp.max(jnp.abs(rows), axis=0)
        code = jnp.ceil(jnp.log2(jnp.maximum(largest, 1e-30)) * STEPS)
        factor = TOP / jnp.exp2(code / STEPS)
        whole = jnp.clip(jnp.round(rows * factor[None]), -TOP, TOP).astype(jnp.int32)
        ref[g * part : (g + 1) * part, at] = whole.reshape(part, width).astype(jnp.int16)
        whole = code.astype(jnp.int32)
        code_rows = whole if g == 0 else jnp.concatenate([code_rows, whole], 0)
    ref[height : height + GROUPS * SUB, at] = code_rows.astype(jnp.int16)


def decode(coded, height):
    width = coded.shape[1]
    part = height // GROUPS
    codes = coded[height : height + GROUPS * SUB].astype(jnp.int32).astype(jnp.float32)
    pieces = []
    for g in range(GROUPS):
        scale = jnp.exp2(codes[g * SUB : (g + 1) * SUB] / STEPS) * (1.0 / TOP)
        rows = coded[g * part : (g + 1) * part].astype(jnp.int32).astype(jnp.float32)
        pieces.append((rows.reshape(part // SUB, SUB, width) * scale[None]).reshape(part, width))
    return jnp.concatenate(pieces, 0)


def near_memory(value):
    return pltpu.with_memory_space_constraint(value, pltpu.VMEM)


def far_memory(value):
    return pltpu.with_memory_space_constraint(value, pltpu.HBM)


def build_kernel(counts_in, columns_in, tiles_in, *refs):
    outs, (counts, columns, tiles, sems) = refs[:-4], refs[-4:]
    copies = [
        pltpu.make_async_copy(source, target, sems.at[k])
        for k, (source, target) in enumerate(
            ((counts_in, counts), (columns_in, columns), (tiles_in, tiles))
        )
    ]
    for copy in copies:
        copy.start()
    for copy in copies:
        copy.wait()
    tall, wide, slots = counts.shape[0], len(outs), tiles.shape[0]
    edge = tiles.shape[1]
    start = jnp.int32(0)
    for i in range(tall):
        count = counts[i]
        for j, out in enumerate(outs):
            slot, found = jnp.int32(0), jnp.int32(0)
            for t in range(wide):
                at = jnp.minimum(start + t, slots - 1)
                hit = (t < count) & (columns[at] == j)
                slot = jnp.where(hit, at, slot)
                found = jnp.where(hit, 1, found)
            tile = tiles[slot].astype(jnp.float32) * found.astype(jnp.float32)
            out[:, i * edge : (i + 1) * edge] = tile.T.astype(jnp.bfloat16)
        start = start + count


def build(tile_values, tile_counts, tile_cols):
    slots, edge, _ = tile_values.shape
    tall = tile_counts.shape[0]
    return pl.pallas_call(
        build_kernel,
        out_shape=[jax.ShapeDtypeStruct((edge, tall * edge), jnp.bfloat16)] * (slots // tall),
        in_specs=[pl.BlockSpec(memory_space=pltpu.HBM)] * 3,
        out_specs=[VMEM] * (slots // tall),
        scratch_shapes=[
            pltpu.SMEM((tall,), jnp.int32),
            pltpu.SMEM((slots,), jnp.int32),
            pltpu.VMEM(tile_values.shape, tile_values.dtype),
            pltpu.SemaphoreType.DMA((3,)),
        ],
        compiler_params=SMALL,
        name="build",
    )(far_memory(tile_counts[:, 0]), far_memory(tile_cols[:, 0]), far_memory(tile_values))


def product_kernel(place, *refs, count, coded):
    blocks, panels, out = refs[:count], refs[count:-1], refs[-1]
    a = jnp.concatenate([b[...] for b in blocks], 0) if count > 1 else blocks[0][...]
    half = out.shape[1]
    step = min(half, 256)
    start = (1 - place[0] if coded else place[0]) * half
    for n in range(0, half, step):
        at = pl.multiple_of(start + n, step)
        value = jnp.concatenate(
            [jnp.dot(a, b[:, pl.ds(at, step)], preferred_element_type=jnp.float32) for b in panels], 0
        )
        if coded:
            encode(value, out, slice(n, n + step))
        else:
            out[:, n : n + step] = value


def products(place, blocks, panels, half, coded):
    height = len(panels) * len(blocks) * blocks[0].shape[0]
    if coded:
        shape = jax.ShapeDtypeStruct((height + GROUPS * SUB, half), jnp.int16)
    else:
        shape = jax.ShapeDtypeStruct((height, half), jnp.float32)
    return pl.pallas_call(
        functools.partial(product_kernel, count=len(blocks), coded=coded),
        out_shape=shape,
        in_specs=[SMEM] + [VMEM] * (len(blocks) + len(panels)),
        out_specs=VMEM,
        compiler_params=SMALL,
        name="leaving" if coded else "staying",
    )(place, *blocks, *panels)


def coded_shape(height, half):
    return jax.ShapeDtypeStruct((height + GROUPS * SUB, half), jnp.int16)


def split_kernel(place, *refs):
    codeds, kept, hold, send = refs[:-3], refs[-3], refs[-2], refs[-1]
    height = kept.shape[0] // 2
    each = kept.shape[0] // len(codeds)
    value = kept[...] + jnp.concatenate([decode(coded[...], each) for coded in codeds], 0)
    first, second = value[:height], value[height:]
    stays = place[1] == 0
    hold[...] = jnp.where(stays, first, second)
    encode(jnp.where(stays, second, first), send)


def split(place, codeds, kept):
    height, half = kept.shape[0] // 2, kept.shape[1]
    return pl.pallas_call(
        split_kernel,
        out_shape=[jax.ShapeDtypeStruct((height, half), jnp.float32), coded_shape(height, half)],
        in_specs=[SMEM] + [VMEM] * (len(codeds) + 1),
        out_specs=[VMEM, VMEM],
        compiler_params=SMALL,
        name="split",
    )(place, *codeds, kept)


def merge_kernel(coded, kept, *outs):
    value = kept[...] + decode(coded[...], kept.shape[0])
    for hold in outs[:-1]:
        hold[...] = value
    encode(value, outs[-1])


def merge(coded, kept, holds):
    height, half = kept.shape
    out = pl.pallas_call(
        merge_kernel,
        out_shape=[jax.ShapeDtypeStruct((height, half), jnp.float32)] * holds + [coded_shape(height, half)],
        in_specs=[VMEM, VMEM],
        out_specs=[VMEM] * (holds + 1),
        compiler_params=SMALL,
        name="merge",
    )(coded, kept)
    return out if holds else (None, out[0])


def finish_kernel(place, kept, coded, *refs, chunks):
    parts, out = refs[:-1], refs[-1]
    pick = place[2]
    height = out.shape[0] // chunks
    own = kept[...] + decode(coded[...], kept.shape[0])
    for j in range(chunks):
        rows = slice(j * height, (j + 1) * height)
        value = own[rows]
        for k in range(len(parts) // (2 * chunks)):
            at = 2 * (k * chunks + j)
            other = decode(parts[at][...], height) + decode(parts[at + 1][...], height)
            value = jnp.where(pick == k + 1, other, value)
        out[rows] = value.astype(jnp.bfloat16)


def finish(place, kept, coded, parts, chunks):
    return pl.pallas_call(
        functools.partial(finish_kernel, chunks=chunks),
        out_shape=jax.ShapeDtypeStruct(kept.shape, jnp.bfloat16),
        in_specs=[SMEM] + [VMEM] * (2 + len(parts)),
        out_specs=VMEM,
        compiler_params=SMALL,
        name="finish",
    )(place, kept, coded, *parts)


def after(value, *others):
    return lax.optimization_barrier((value, *others))[0]


def solution(mesh):
    rows, cols = mesh.shape["row"], mesh.shape["col"]
    spread = rows // cols
    assert spread == 2 and rows & (rows - 1) == 0 and cols >= 4

    def permute(value, move):
        pairs = [
            (r * cols + c, to[0] * cols + to[1])
            for r in range(rows)
            for c in range(cols)
            if (to := move(r, c)) is not None
        ]
        return lax.ppermute(value, ("row", "col"), pairs)

    last = cols // 2

    last = cols // 2
    inner = last - 2

    def met(r, c, bits):
        return not ((r // spread) ^ c) & bits

    def across(value):
        return permute(value, lambda r, c: (r ^ 1, c))

    def along(value):
        return permute(value, lambda r, c: (r ^ spread, c))

    def folded(got, hold):
        bit = 2
        while bit < last:
            hold, send = merge(got, hold, 1)
            got = permute(
                send,
                lambda r, c: (r ^ (bit * spread), c) if met(r, c, bit - 2) and not met(r, c, bit) else None,
            )
            bit *= 2
        return got, hold

    def body(tile_values, tile_counts, tile_cols, panels):
        half = panels.shape[1] // spread
        r, c = lax.axis_index("row"), lax.axis_index("col")
        q = r // spread
        place = jnp.stack([r % spread, (q + c) % 2, (q ^ c) // 2]).astype(jnp.int32)
        other = near_memory(permute(panels, lambda r, c: (r, c ^ 1)))
        panels = near_memory(panels)

        own = [near_memory(block) for block in build(tile_values, tile_counts, tile_cols)]
        chunks = len(own)
        dense = {0: own}
        bit = last
        while bit > 1:
            for m in list(dense):
                blocks = []
                for j in range(chunks):
                    blocks.append(near_memory(permute(dense[m][j], lambda r, c: (r, c ^ bit))))
                dense[m ^ bit] = blocks
            bit //= 2
        moved = [m for m in sorted(dense) if m]

        first = products(place, own, [panels], half, True)
        sent = [across(first)]
        second = products(place, own, [after(other, first)], half, True)
        sent.append(across(second))
        kept = products(place, own, [after(panels, second), other], half, False)
        coded, stay = {}, {}

        def multiply(j, order):
            for m in moved:
                block = after(dense[m][j], order)
                code = products(place, [block], [panels, other], half, True)
                coded[m, j] = across(code)
                stay[m, j] = products(place, [after(block, code)], [panels, other], half, False)

        multiply(0, kept)
        hold, send = split(place, [sent[0], after(sent[1], stay[moved[0], 0])], kept)
        got = along(send)
        for j in range(1, chunks):
            multiply(j, send)

        parts = {}
        order = send
        for j in range(chunks):
            for m in moved:
                part_hold, part_send = split(place, [after(coded[m, j], order)], stay[m, j])
                part_got, part_hold = folded(along(part_send), part_hold)
                if j == 1:
                    order = part_send
                _, code = merge(part_got, part_hold, 0)
                if j == 0:
                    near = permute(code, lambda r, c: (r, c ^ m) if met(r, c, inner) else None)
                    far = permute(
                        near,
                        lambda r, c: (r ^ (last * spread), c)
                        if met(r, c ^ m, inner) and not met(r, c ^ m, last)
                        else None,
                    )
                else:
                    far = permute(
                        code,
                        lambda r, c: (r ^ (last * spread), c ^ m)
                        if met(r, c, inner) and not met(r, c, last)
                        else None,
                    )
                    near = permute(code, lambda r, c: (r, c ^ m) if met(r, c, inner | last) else None)
                parts[m, j] = [near, far]
        got, hold = folded(got, hold)
        hold, send = merge(got, hold, 1)
        got = permute(
            send,
            lambda r, c: (r ^ (last * spread), c) if met(r, c, inner) and not met(r, c, last) else None,
        )
        pieces = [x for m in moved for j in range(chunks) for x in parts[m, j]]
        return finish(place, hold, got, pieces, chunks)

    return jax.shard_map(
        body,
        mesh=mesh,
        in_specs=(P("row", "col", None), P("row", "col"), P("row", "col"), P("row", "col")),
        out_specs=P("col", "row"),
        check_vma=False,
    )
```

```python
import functools

import jax
import jax.numpy as jnp
from jax import lax
from jax.experimental import pallas as pl
from jax.experimental.pallas import tpu as pltpu
from jax.sharding import PartitionSpec as P


GROUPS = 2
SUB = 8
TOP = 32767.0
STEPS = 128.0
VMEM = pl.BlockSpec(memory_space=pltpu.VMEM)
SMALL = pltpu.CompilerParams(vmem_limit_bytes=16 * 2**20)


def encode(value, ref, at=slice(None)):
    height, width = value.shape
    part = height // GROUPS
    for g in range(GROUPS):
        rows = value[g * part : (g + 1) * part].reshape(part // SUB, SUB, width)
        largest = jnp.max(jnp.abs(rows), axis=0)
        code = jnp.ceil(jnp.log2(jnp.maximum(largest, 1e-30)) * STEPS)
        factor = TOP / jnp.exp2(code / STEPS)
        whole = jnp.clip(jnp.round(rows * factor[None]), -TOP, TOP).astype(jnp.int32)
        ref[g * part : (g + 1) * part, at] = whole.reshape(part, width).astype(jnp.int16)
        whole = code.astype(jnp.int32)
        code_rows = whole if g == 0 else jnp.concatenate([code_rows, whole], 0)
    ref[height : height + GROUPS * SUB, at] = code_rows.astype(jnp.int16)


def decode(coded, height):
    width = coded.shape[1]
    part = height // GROUPS
    codes = coded[height : height + GROUPS * SUB].astype(jnp.int32).astype(jnp.float32)
    pieces = []
    for g in range(GROUPS):
        scale = jnp.exp2(codes[g * SUB : (g + 1) * SUB] / STEPS) * (1.0 / TOP)
        rows = coded[g * part : (g + 1) * part].astype(jnp.int32).astype(jnp.float32)
        pieces.append((rows.reshape(part // SUB, SUB, width) * scale[None]).reshape(part, width))
    return jnp.concatenate(pieces, 0)


def places(spread):
    r, c = lax.axis_index("row"), lax.axis_index("col")
    q = r // spread
    return r % spread, (q + c) % 2, (q // 2) ^ (c // 2)


def near_memory(value):
    return pltpu.with_memory_space_constraint(value, pltpu.VMEM)


def far_memory(value):
    return pltpu.with_memory_space_constraint(value, pltpu.HBM)


def build_kernel(counts_in, columns_in, tiles_in, panels_in, *refs):
    outs, (panels, counts, columns, tiles, sems) = refs[:-5], refs[-5:]
    copies = [
        pltpu.make_async_copy(source, target, sems.at[k])
        for k, (source, target) in enumerate(
            ((counts_in, counts), (columns_in, columns), (tiles_in, tiles), (panels_in, panels))
        )
    ]
    for copy in copies:
        copy.start()
    for copy in copies[:-1]:
        copy.wait()
    tall, wide, slots = counts.shape[0], len(outs), tiles.shape[0]
    edge = tiles.shape[1]
    start = jnp.int32(0)
    for i in range(tall):
        count = counts[i]
        for j, out in enumerate(outs):
            slot, found = jnp.int32(0), jnp.int32(0)
            for t in range(wide):
                at = jnp.minimum(start + t, slots - 1)
                hit = (t < count) & (columns[at] == j)
                slot = jnp.where(hit, at, slot)
                found = jnp.where(hit, 1, found)
            tile = tiles[slot].astype(jnp.float32) * found.astype(jnp.float32)
            out[:, i * edge : (i + 1) * edge] = tile.T.astype(jnp.bfloat16)
        start = start + count
    copies[-1].wait()


def build(tile_values, tile_counts, tile_cols, panels):
    slots, edge, _ = tile_values.shape
    tall = tile_counts.shape[0]
    return pl.pallas_call(
        build_kernel,
        out_shape=[jax.ShapeDtypeStruct((edge, tall * edge), jnp.bfloat16)] * (slots // tall)
        + [jax.ShapeDtypeStruct(panels.shape, panels.dtype)],
        in_specs=[pl.BlockSpec(memory_space=pltpu.HBM)] * 4,
        out_specs=[VMEM] * (slots // tall + 1),
        scratch_shapes=[
            pltpu.SMEM((tall,), jnp.int32),
            pltpu.SMEM((slots,), jnp.int32),
            pltpu.VMEM(tile_values.shape, tile_values.dtype),
            pltpu.SemaphoreType.DMA((4,)),
        ],
        compiler_params=SMALL,
        name="build",
    )(far_memory(tile_counts[:, 0]), far_memory(tile_cols[:, 0]), far_memory(tile_values), far_memory(panels))


def product_kernel(*refs, count, coded, spread):
    blocks, panels, out = refs[:count], refs[count:-1], refs[-1]
    a = jnp.concatenate([b[...] for b in blocks], 0) if count > 1 else blocks[0][...]
    half = out.shape[1]
    step = min(half, 256)
    side = places(spread)[0]
    start = (1 - side if coded else side) * half
    for n in range(0, half, step):
        at = pl.multiple_of(start + n, step)
        value = jnp.concatenate(
            [jnp.dot(a, b[:, pl.ds(at, step)], preferred_element_type=jnp.float32) for b in panels], 0
        )
        if coded:
            encode(value, out, slice(n, n + step))
        else:
            out[:, n : n + step] = value


def products(blocks, panels, half, coded):
    height = len(panels) * len(blocks) * blocks[0].shape[0]
    if coded:
        shape = jax.ShapeDtypeStruct((height + GROUPS * SUB, half), jnp.int16)
    else:
        shape = jax.ShapeDtypeStruct((height, half), jnp.float32)
    return pl.pallas_call(
        functools.partial(
            product_kernel, count=len(blocks), coded=coded, spread=panels[0].shape[1] // half
        ),
        out_shape=shape,
        in_specs=[VMEM] * (len(blocks) + len(panels)),
        out_specs=VMEM,
        compiler_params=SMALL,
        name="leaving" if coded else "staying",
    )(*blocks, *panels)


def coded_shape(height, half):
    return jax.ShapeDtypeStruct((height + GROUPS * SUB, half), jnp.int16)


def split_kernel(*refs, spread):
    codeds, kept, hold, send = refs[:-3], refs[-3], refs[-2], refs[-1]
    height = kept.shape[0] // 2
    each = kept.shape[0] // len(codeds)
    value = kept[...] + jnp.concatenate([decode(coded[...], each) for coded in codeds], 0)
    first, second = value[:height], value[height:]
    stays = places(spread)[1] == 0
    hold[...] = jnp.where(stays, first, second)
    encode(jnp.where(stays, second, first), send)


def split(codeds, kept, spread):
    height, half = kept.shape[0] // 2, kept.shape[1]
    return pl.pallas_call(
        functools.partial(split_kernel, spread=spread),
        out_shape=[jax.ShapeDtypeStruct((height, half), jnp.float32), coded_shape(height, half)],
        in_specs=[VMEM] * (len(codeds) + 1),
        out_specs=[VMEM, VMEM],
        compiler_params=SMALL,
        name="split",
    )(*codeds, kept)


def merge_kernel(coded, kept, *outs):
    value = kept[...] + decode(coded[...], kept.shape[0])
    for hold in outs[:-1]:
        hold[...] = value
    encode(value, outs[-1])


def merge(coded, kept, holds):
    height, half = kept.shape
    out = pl.pallas_call(
        merge_kernel,
        out_shape=[jax.ShapeDtypeStruct((height, half), jnp.float32)] * holds + [coded_shape(height, half)],
        in_specs=[VMEM, VMEM],
        out_specs=[VMEM] * (holds + 1),
        compiler_params=SMALL,
        name="merge",
    )(coded, kept)
    return out if holds else (None, out[0])


def finish_kernel(kept, coded, *refs, chunks, spread):
    parts, out = refs[:-1], refs[-1]
    pick = places(spread)[2]
    height = out.shape[0] // chunks
    own = kept[...] + decode(coded[...], kept.shape[0])
    for j in range(chunks):
        rows = slice(j * height, (j + 1) * height)
        value = own[rows]
        for k in range(len(parts) // (2 * chunks)):
            at = 2 * (k * chunks + j)
            other = decode(parts[at][...], height) + decode(parts[at + 1][...], height)
            value = jnp.where(pick == k + 1, other, value)
        out[rows] = value.astype(jnp.bfloat16)


def finish(kept, coded, parts, chunks, spread):
    return pl.pallas_call(
        functools.partial(finish_kernel, chunks=chunks, spread=spread),
        out_shape=jax.ShapeDtypeStruct(kept.shape, jnp.bfloat16),
        in_specs=[VMEM] * (2 + len(parts)),
        out_specs=VMEM,
        compiler_params=SMALL,
        name="finish",
    )(kept, coded, *parts)


def after(value, *others):
    return lax.optimization_barrier((value, *others))[0]


def solution(mesh):
    rows, cols = mesh.shape["row"], mesh.shape["col"]
    spread = rows // cols
    assert spread == 2 and rows & (rows - 1) == 0 and cols >= 4

    def permute(value, move):
        pairs = [
            (r * cols + c, to[0] * cols + to[1])
            for r in range(rows)
            for c in range(cols)
            if (to := move(r, c)) is not None
        ]
        return lax.ppermute(value, ("row", "col"), pairs)

    last = cols // 2

    last = cols // 2
    inner = last - 2

    def met(r, c, bits):
        return not ((r // spread) ^ c) & bits

    def across(value):
        return permute(value, lambda r, c: (r ^ 1, c))

    def along(value):
        return permute(value, lambda r, c: (r ^ spread, c))

    def folded(got, hold):
        bit = 2
        while bit < last:
            hold, send = merge(got, hold, 1)
            got = permute(
                send,
                lambda r, c: (r ^ (bit * spread), c) if met(r, c, bit - 2) and not met(r, c, bit) else None,
            )
            bit *= 2
        return got, hold

    def body(tile_values, tile_counts, tile_cols, panels):
        half = panels.shape[1] // spread
        other = near_memory(permute(panels, lambda r, c: (r, c ^ 1)))
        *own, panels = [near_memory(x) for x in build(tile_values, tile_counts, tile_cols, panels)]
        chunks = len(own)
        dense = {0: own}
        bit = last
        while bit > 1:
            for m in list(dense):
                blocks = []
                for j in range(chunks):
                    blocks.append(near_memory(permute(dense[m][j], lambda r, c: (r, c ^ bit))))
                dense[m ^ bit] = blocks
            bit //= 2
        moved = [m for m in sorted(dense) if m]

        first = products(own, [panels], half, True)
        sent = [across(first)]
        second = products(own, [after(other, first)], half, True)
        sent.append(across(second))
        kept = products(own, [after(panels, second), other], half, False)
        coded, stay = {}, {}

        def multiply(j, order):
            for m in moved:
                block = after(dense[m][j], order)
                code = products([block], [panels, other], half, True)
                coded[m, j] = across(code)
                stay[m, j] = products([after(block, code)], [panels, other], half, False)

        multiply(0, kept)
        hold, send = split([sent[0], after(sent[1], stay[moved[0], 0])], kept, spread)
        got = along(send)
        for j in range(1, chunks):
            multiply(j, send)

        parts = {}
        order = stay[moved[-1], chunks - 1]
        for j in range(chunks):
            for m in moved:
                part_hold, part_send = split([after(coded[m, j], order)], stay[m, j], spread)
                part_got, part_hold = folded(along(part_send), part_hold)
                if j == 0 and m == moved[0]:
                    got, hold = folded(got, hold)
                    hold, send = merge(after(got, part_send), hold, 1)
                    got = permute(
                        send,
                        lambda r, c: (r ^ (last * spread), c)
                        if met(r, c, inner) and not met(r, c, last)
                        else None,
                    )
                _, code = merge(after(part_got, send), part_hold, 0)
                order = code
                if j == 0:
                    near = permute(code, lambda r, c: (r, c ^ m) if met(r, c, inner) else None)
                    far = permute(
                        near,
                        lambda r, c: (r ^ (last * spread), c)
                        if met(r, c ^ m, inner) and not met(r, c ^ m, last)
                        else None,
                    )
                else:
                    far = permute(
                        code,
                        lambda r, c: (r ^ (last * spread), c ^ m)
                        if met(r, c, inner) and not met(r, c, last)
                        else None,
                    )
                    near = permute(code, lambda r, c: (r, c ^ m) if met(r, c, inner | last) else None)
                parts[m, j] = [near, far]
        pieces = [x for m in moved for j in range(chunks) for x in parts[m, j]]
        return finish(hold, got, pieces, chunks, spread)

    return jax.shard_map(
        body,
        mesh=mesh,
        in_specs=(P("row", "col", None), P("row", "col"), P("row", "col"), P("row", "col")),
        out_specs=P("col", "row"),
        check_vma=False,
    )
```

```python
import functools

import jax
import jax.numpy as jnp
from jax import lax
from jax.experimental import pallas as pl
from jax.experimental.pallas import tpu as pltpu
from jax.sharding import PartitionSpec as P


GROUPS = 2
SUB = 8
TOP = 32767.0
STEPS = 128.0
VMEM = pl.BlockSpec(memory_space=pltpu.VMEM)
SMALL = pltpu.CompilerParams(vmem_limit_bytes=16 * 2**20)


def encode(value, ref, at=slice(None)):
    height, width = value.shape
    part = height // GROUPS
    for g in range(GROUPS):
        rows = value[g * part : (g + 1) * part].reshape(part // SUB, SUB, width)
        largest = jnp.max(jnp.abs(rows), axis=0)
        code = jnp.ceil(jnp.log2(jnp.maximum(largest, 1e-30)) * STEPS)
        factor = TOP / jnp.exp2(code / STEPS)
        whole = jnp.clip(jnp.round(rows * factor[None]), -TOP, TOP).astype(jnp.int32)
        ref[g * part : (g + 1) * part, at] = whole.reshape(part, width).astype(jnp.int16)
        whole = code.astype(jnp.int32)
        code_rows = whole if g == 0 else jnp.concatenate([code_rows, whole], 0)
    ref[height : height + GROUPS * SUB, at] = code_rows.astype(jnp.int16)


def decode(coded, height):
    width = coded.shape[1]
    part = height // GROUPS
    codes = coded[height : height + GROUPS * SUB].astype(jnp.int32).astype(jnp.float32)
    pieces = []
    for g in range(GROUPS):
        scale = jnp.exp2(codes[g * SUB : (g + 1) * SUB] / STEPS) * (1.0 / TOP)
        rows = coded[g * part : (g + 1) * part].astype(jnp.int32).astype(jnp.float32)
        pieces.append((rows.reshape(part // SUB, SUB, width) * scale[None]).reshape(part, width))
    return jnp.concatenate(pieces, 0)


def places(spread):
    r, c = lax.axis_index("row"), lax.axis_index("col")
    q = r // spread
    return r % spread, (q + c) % 2, (q // 2) ^ (c // 2)


def near_memory(value):
    return pltpu.with_memory_space_constraint(value, pltpu.VMEM)


def far_memory(value):
    return pltpu.with_memory_space_constraint(value, pltpu.HBM)


def build_kernel(counts_in, columns_in, tiles_in, panels_in, *refs):
    outs, (panels, counts, columns, tiles, sems) = refs[:-5], refs[-5:]
    copies = [
        pltpu.make_async_copy(source, target, sems.at[k])
        for k, (source, target) in enumerate(
            ((counts_in, counts), (columns_in, columns), (tiles_in, tiles), (panels_in, panels))
        )
    ]
    for copy in copies:
        copy.start()
    for copy in copies[:-1]:
        copy.wait()
    tall, wide, slots = counts.shape[0], len(outs), tiles.shape[0]
    edge = tiles.shape[1]
    start = jnp.int32(0)
    for i in range(tall):
        count = counts[i]
        for j, out in enumerate(outs):
            slot, found = jnp.int32(0), jnp.int32(0)
            for t in range(wide):
                at = jnp.minimum(start + t, slots - 1)
                hit = (t < count) & (columns[at] == j)
                slot = jnp.where(hit, at, slot)
                found = jnp.where(hit, 1, found)
            tile = tiles[slot].astype(jnp.float32) * found.astype(jnp.float32)
            out[:, i * edge : (i + 1) * edge] = tile.T.astype(jnp.bfloat16)
        start = start + count
    copies[-1].wait()


def build(tile_values, tile_counts, tile_cols, panels):
    slots, edge, _ = tile_values.shape
    tall = tile_counts.shape[0]
    return pl.pallas_call(
        build_kernel,
        out_shape=[jax.ShapeDtypeStruct((edge, tall * edge), jnp.bfloat16)] * (slots // tall)
        + [jax.ShapeDtypeStruct(panels.shape, panels.dtype)],
        in_specs=[pl.BlockSpec(memory_space=pltpu.HBM)] * 4,
        out_specs=[VMEM] * (slots // tall + 1),
        scratch_shapes=[
            pltpu.SMEM((tall,), jnp.int32),
            pltpu.SMEM((slots,), jnp.int32),
            pltpu.VMEM(tile_values.shape, tile_values.dtype),
            pltpu.SemaphoreType.DMA((4,)),
        ],
        compiler_params=SMALL,
        name="build",
    )(far_memory(tile_counts[:, 0]), far_memory(tile_cols[:, 0]), far_memory(tile_values), far_memory(panels))


def product_kernel(*refs, count, coded, spread):
    blocks, panels, out = refs[:count], refs[count:-1], refs[-1]
    a = jnp.concatenate([b[...] for b in blocks], 0) if count > 1 else blocks[0][...]
    half = out.shape[1]
    step = min(half, 256)
    side = places(spread)[0]
    start = (1 - side if coded else side) * half
    for n in range(0, half, step):
        at = pl.multiple_of(start + n, step)
        value = jnp.concatenate(
            [jnp.dot(a, b[:, pl.ds(at, step)], preferred_element_type=jnp.float32) for b in panels], 0
        )
        if coded:
            encode(value, out, slice(n, n + step))
        else:
            out[:, n : n + step] = value


def products(blocks, panels, half, coded):
    height = len(panels) * len(blocks) * blocks[0].shape[0]
    if coded:
        shape = jax.ShapeDtypeStruct((height + GROUPS * SUB, half), jnp.int16)
    else:
        shape = jax.ShapeDtypeStruct((height, half), jnp.float32)
    return pl.pallas_call(
        functools.partial(
            product_kernel, count=len(blocks), coded=coded, spread=panels[0].shape[1] // half
        ),
        out_shape=shape,
        in_specs=[VMEM] * (len(blocks) + len(panels)),
        out_specs=VMEM,
        compiler_params=SMALL,
        name="leaving" if coded else "staying",
    )(*blocks, *panels)


def coded_shape(height, half):
    return jax.ShapeDtypeStruct((height + GROUPS * SUB, half), jnp.int16)


def split_kernel(*refs, spread):
    codeds, kept, hold, send = refs[:-3], refs[-3], refs[-2], refs[-1]
    height = kept.shape[0] // 2
    each = kept.shape[0] // len(codeds)
    value = kept[...] + jnp.concatenate([decode(coded[...], each) for coded in codeds], 0)
    first, second = value[:height], value[height:]
    stays = places(spread)[1] == 0
    hold[...] = jnp.where(stays, first, second)
    encode(jnp.where(stays, second, first), send)


def split(codeds, kept, spread):
    height, half = kept.shape[0] // 2, kept.shape[1]
    return pl.pallas_call(
        functools.partial(split_kernel, spread=spread),
        out_shape=[jax.ShapeDtypeStruct((height, half), jnp.float32), coded_shape(height, half)],
        in_specs=[VMEM] * (len(codeds) + 1),
        out_specs=[VMEM, VMEM],
        compiler_params=SMALL,
        name="split",
    )(*codeds, kept)


def merge_kernel(coded, kept, *outs):
    value = kept[...] + decode(coded[...], kept.shape[0])
    for hold in outs[:-1]:
        hold[...] = value
    encode(value, outs[-1])


def merge(coded, kept, holds):
    height, half = kept.shape
    out = pl.pallas_call(
        merge_kernel,
        out_shape=[jax.ShapeDtypeStruct((height, half), jnp.float32)] * holds + [coded_shape(height, half)],
        in_specs=[VMEM, VMEM],
        out_specs=[VMEM] * (holds + 1),
        compiler_params=SMALL,
        name="merge",
    )(coded, kept)
    return out if holds else (None, out[0])


def finish_kernel(kept, coded, *refs, chunks, spread):
    parts, out = refs[:-1], refs[-1]
    pick = places(spread)[2]
    height = out.shape[0] // chunks
    own = kept[...] + decode(coded[...], kept.shape[0])
    for j in range(chunks):
        rows = slice(j * height, (j + 1) * height)
        value = own[rows]
        for k in range(len(parts) // (2 * chunks)):
            at = 2 * (k * chunks + j)
            other = decode(parts[at][...], height) + decode(parts[at + 1][...], height)
            value = jnp.where(pick == k + 1, other, value)
        out[rows] = value.astype(jnp.bfloat16)


def finish(kept, coded, parts, chunks, spread):
    return pl.pallas_call(
        functools.partial(finish_kernel, chunks=chunks, spread=spread),
        out_shape=jax.ShapeDtypeStruct(kept.shape, jnp.bfloat16),
        in_specs=[VMEM] * (2 + len(parts)),
        out_specs=VMEM,
        compiler_params=SMALL,
        name="finish",
    )(kept, coded, *parts)


def chosen_kernel(block, *refs, coded, spread):
    panels, out = refs[:-1], refs[-1]
    width = out.shape[1]
    step = min(width, 256)
    stays = places(spread)[1]
    for k, panel in enumerate(panels):

        @pl.when(stays == (1 - k if coded else k))
        def _():
            for n in range(0, width, step):
                at = slice(n, n + step)
                value = jnp.dot(block[...], panel[:, at], preferred_element_type=jnp.float32)
                if coded:
                    encode(value, out, at)
                else:
                    out[:, at] = value


def chosen(block, panels, spread, coded):
    height, width = block.shape[0], panels[0].shape[1]
    return pl.pallas_call(
        functools.partial(chosen_kernel, coded=coded, spread=spread),
        out_shape=coded_shape(height, width) if coded else jax.ShapeDtypeStruct((height, width), jnp.float32),
        in_specs=[VMEM] * 3,
        out_specs=VMEM,
        compiler_params=SMALL,
        name="chosen",
    )(block, *panels)


def halve_kernel(coded, kept, hold, send, *, spread):
    height, half = hold.shape
    side = places(spread)[0]

    def value(which):
        at = pl.ds(pl.multiple_of(which * half, half), half)
        return kept[:, at] + decode(coded[:, at], height)

    encode(value(1 - side), send)
    hold[...] = value(side)


def halve(coded, kept, spread):
    height, half = kept.shape[0], kept.shape[1] // spread
    return pl.pallas_call(
        functools.partial(halve_kernel, spread=spread),
        out_shape=[jax.ShapeDtypeStruct((height, half), jnp.float32), coded_shape(height, half)],
        in_specs=[VMEM, VMEM],
        out_specs=[VMEM, VMEM],
        compiler_params=SMALL,
        name="halve",
    )(coded, kept)


def join_kernel(*refs):
    count = (len(refs) - 2) // 2
    value = jnp.concatenate(
        [kept[...] + decode(coded[...], kept.shape[0]) for coded, kept in zip(refs[:count], refs[count:-2])], 0
    )
    refs[-2][...] = value
    encode(value, refs[-1])


def join(codeds, kepts):
    height, half = sum(kept.shape[0] for kept in kepts), kepts[0].shape[1]
    return pl.pallas_call(
        join_kernel,
        out_shape=[jax.ShapeDtypeStruct((height, half), jnp.float32), coded_shape(height, half)],
        in_specs=[VMEM] * (2 * len(kepts)),
        out_specs=[VMEM, VMEM],
        compiler_params=SMALL,
        name="join",
    )(*codeds, *kepts)


def after(value, *others):
    return lax.optimization_barrier((value, *others))[0]


def solution(mesh):
    rows, cols = mesh.shape["row"], mesh.shape["col"]
    spread = rows // cols
    assert spread == 2 and rows & (rows - 1) == 0 and cols >= 4

    def permute(value, move):
        pairs = [
            (r * cols + c, to[0] * cols + to[1])
            for r in range(rows)
            for c in range(cols)
            if (to := move(r, c)) is not None
        ]
        return lax.ppermute(value, ("row", "col"), pairs)

    last = cols // 2

    last = cols // 2
    inner = last - 2

    def met(r, c, bits):
        return not ((r // spread) ^ c) & bits

    def across(value):
        return permute(value, lambda r, c: (r ^ 1, c))

    def along(value):
        return permute(value, lambda r, c: (r ^ spread, c))

    def folded(got, hold):
        bit = 2
        while bit < last:
            hold, send = merge(got, hold, 1)
            got = permute(
                send,
                lambda r, c: (r ^ (bit * spread), c) if met(r, c, bit - 2) and not met(r, c, bit) else None,
            )
            bit *= 2
        return got, hold

    def body(tile_values, tile_counts, tile_cols, panels):
        half = panels.shape[1] // spread
        other = near_memory(permute(panels, lambda r, c: (r, c ^ 1)))
        *own, panels = [near_memory(x) for x in build(tile_values, tile_counts, tile_cols, panels)]
        chunks = len(own)
        dense = {0: own}
        bit = last
        while bit > 1:
            for m in list(dense):
                blocks = []
                for j in range(chunks):
                    blocks.append(near_memory(permute(dense[m][j], lambda r, c: (r, c ^ bit))))
                dense[m ^ bit] = blocks
            bit //= 2
        moved = [m for m in sorted(dense) if m]

        both = [panels, other]
        code_a = products(own[:1], both, half, True)
        got_a = across(code_a)
        order = code_a
        gots_b, stays_b = [], []
        for block in own[1:]:
            order = chosen(after(block, order), both, spread, True)
            gots_b.append(along(order))
        stay_a = products([after(own[0], order)], both, half, False)
        order = stay_a
        for block in own[1:]:
            order = chosen(after(block, order), both, spread, False)
            stays_b.append(order)
        coded, stay = {}, {}

        def leave(j, order):
            for m in moved:
                order = products([after(dense[m][j], order)], both, half, True)
                coded[m, j] = across(order)
            return order

        def keep(j, order):
            for m in moved:
                order = stay[m, j] = products([after(dense[m][j], order)], both, half, False)
            return order

        order = leave(0, order)
        hold, send = split([after(got_a, order)], stay_a, spread)
        holds, gots, order = [hold], [along(send)], send
        for got_b, stay_b in zip(gots_b, stays_b):
            hold, send = halve(after(got_b, order), stay_b, spread)
            holds.append(hold)
            gots.append(across(send))
            order = send
        order = keep(0, order)
        hold, send = join([after(gots[0], order), *gots[1:]], holds)
        bit = 2
        while bit < last:
            got = permute(
                send,
                lambda r, c: (r ^ (bit * spread), c) if met(r, c, bit - 2) and not met(r, c, bit) else None,
            )
            hold, send = merge(got, hold, 1)
            bit *= 2
        got = permute(send, lambda r, c: (r ^ (last * spread), c) if met(r, c, inner) and not met(r, c, last) else None)
        order = send
        for j in range(1, chunks):
            order = keep(j, leave(j, order))

        parts = {}
        for j in range(chunks):
            for m in moved:
                part_hold, order = split([after(coded[m, j], order)], stay[m, j], spread)
                part_got, part_hold = folded(along(order), part_hold)
                _, order = merge(part_got, part_hold, 0)
                if j == 0:
                    near = permute(order, lambda r, c: (r, c ^ m) if met(r, c, inner) else None)
                    far = permute(
                        near,
                        lambda r, c: (r ^ (last * spread), c)
                        if met(r, c ^ m, inner) and not met(r, c ^ m, last)
                        else None,
                    )
                else:
                    far = permute(
                        order,
                        lambda r, c: (r ^ (last * spread), c ^ m)
                        if met(r, c, inner) and not met(r, c, last)
                        else None,
                    )
                    near = permute(order, lambda r, c: (r, c ^ m) if met(r, c, inner | last) else None)
                parts[m, j] = [near, far]
        pieces = [x for m in moved for j in range(chunks) for x in parts[m, j]]
        return finish(hold, got, pieces, chunks, spread)

    return jax.shard_map(
        body,
        mesh=mesh,
        in_specs=(P("row", "col", None), P("row", "col"), P("row", "col"), P("row", "col")),
        out_specs=P("col", "row"),
        check_vma=False,
    )
```

```python
import functools

import jax
import jax.numpy as jnp
from jax import lax
from jax.experimental import pallas as pl
from jax.experimental.pallas import tpu as pltpu
from jax.sharding import PartitionSpec as P


GROUPS = 1
SUB = 8
TOP = 32767.0
STEPS = 128.0
VMEM = pl.BlockSpec(memory_space=pltpu.VMEM)
SMALL = pltpu.CompilerParams(vmem_limit_bytes=16 * 2**20)


def encode(value, ref, at=slice(None)):
    height, width = value.shape
    part = height // GROUPS
    for g in range(GROUPS):
        rows = value[g * part : (g + 1) * part].reshape(part // SUB, SUB, width)
        largest = jnp.max(jnp.abs(rows), axis=0)
        code = jnp.ceil(jnp.log2(jnp.maximum(largest, 1e-30)) * STEPS)
        factor = TOP / jnp.exp2(code / STEPS)
        whole = jnp.clip(jnp.round(rows * factor[None]), -TOP, TOP).astype(jnp.int32)
        ref[g * part : (g + 1) * part, at] = whole.reshape(part, width).astype(jnp.int16)
        whole = code.astype(jnp.int32)
        code_rows = whole if g == 0 else jnp.concatenate([code_rows, whole], 0)
    ref[height : height + GROUPS * SUB, at] = code_rows.astype(jnp.int16)


def decode(coded, height):
    width = coded.shape[1]
    part = height // GROUPS
    codes = coded[height : height + GROUPS * SUB].astype(jnp.int32).astype(jnp.float32)
    pieces = []
    for g in range(GROUPS):
        scale = jnp.exp2(codes[g * SUB : (g + 1) * SUB] / STEPS) * (1.0 / TOP)
        rows = coded[g * part : (g + 1) * part].astype(jnp.int32).astype(jnp.float32)
        pieces.append((rows.reshape(part // SUB, SUB, width) * scale[None]).reshape(part, width))
    return jnp.concatenate(pieces, 0)


def places(spread):
    r, c = lax.axis_index("row"), lax.axis_index("col")
    q = r // spread
    return r % spread, (q + c) % 2, (q // 2) ^ (c // 2)


def near_memory(value):
    return pltpu.with_memory_space_constraint(value, pltpu.VMEM)


def far_memory(value):
    return pltpu.with_memory_space_constraint(value, pltpu.HBM)


FIRST = {"a": "x", "b": "z", "0": "xz", "1": "xz"}
OWN = ("a", "b")
PARTS = (144, 112)
TURN = ("0",)
PLAN = (
    "leave_a",
    "first_a",
    "leave_b",
    "first_b",
    "stay_a",
    "stay_b",
    "leave_0",
    "first_0",
    "split_a",
    "second_a",
    "split_b",
    "second_b",
    "stay_0",
    "leave_1",
    "first_1",
    "stay_1",
    "code_0",
    "near_0",
    "code_a",
    "far_a",
    "code_b",
    "far_b",
    "far_0",
    "code_1",
    "near_1",
    "far_1",
)
KERNELS = ("leave", "stay", "split", "code")


def build_kernel(counts_in, columns_in, tiles_in, panels_in, *refs):
    outs, (panels, counts, columns, tiles, sems) = refs[:-5], refs[-5:]
    copies = [
        pltpu.make_async_copy(source, target, sems.at[k])
        for k, (source, target) in enumerate(
            ((counts_in, counts), (columns_in, columns), (tiles_in, tiles), (panels_in, panels))
        )
    ]
    for copy in copies:
        copy.start()
    for copy in copies[:-1]:
        copy.wait()
    tall, slots = counts.shape[0], tiles.shape[0]
    wide = slots // tall
    edge = tiles.shape[1]
    start = jnp.int32(0)
    for i in range(tall):
        count = counts[i]
        for j in range(wide):
            slot, found = jnp.int32(0), jnp.int32(0)
            for t in range(wide):
                at = jnp.minimum(start + t, slots - 1)
                hit = (t < count) & (columns[at] == j)
                slot = jnp.where(hit, at, slot)
                found = jnp.where(hit, 1, found)
            tile = tiles[slot].astype(jnp.float32) * found.astype(jnp.float32)
            tile = tile.T.astype(jnp.bfloat16)
            at = slice(i * edge, (i + 1) * edge)
            outs[j][:, at] = tile
            top = 0
            for out in outs[wide:]:
                low, high = max(top, j * edge), min(top + out.shape[0], (j + 1) * edge)
                if low < high:
                    out[low - top : high - top, at] = tile[low - j * edge : high - j * edge]
                top += out.shape[0]
        start = start + count
    copies[-1].wait()


def build(tile_values, tile_counts, tile_cols, panels):
    slots, edge, _ = tile_values.shape
    tall = tile_counts.shape[0]
    wide = slots // tall
    heights = [edge] * wide + [part * edge // 128 for part in PARTS]
    return pl.pallas_call(
        build_kernel,
        out_shape=[jax.ShapeDtypeStruct((height, tall * edge), jnp.bfloat16) for height in heights]
        + [jax.ShapeDtypeStruct(panels.shape, panels.dtype)],
        in_specs=[pl.BlockSpec(memory_space=pltpu.HBM)] * 4,
        out_specs=[VMEM] * (len(heights) + 1),
        scratch_shapes=[
            pltpu.SMEM((tall,), jnp.int32),
            pltpu.SMEM((slots,), jnp.int32),
            pltpu.VMEM(tile_values.shape, tile_values.dtype),
            pltpu.SemaphoreType.DMA((4,)),
        ],
        compiler_params=SMALL,
        name="build",
    )(far_memory(tile_counts[:, 0]), far_memory(tile_cols[:, 0]), far_memory(tile_values), far_memory(panels))


def product_kernel(*refs, count, coded, spread):
    blocks, panels, out = refs[:count], refs[count:-1], refs[-1]
    a = jnp.concatenate([b[...] for b in blocks], 0) if count > 1 else blocks[0][...]
    half = out.shape[1]
    step = min(half, 256)
    side = places(spread)[0]
    start = (1 - side if coded else side) * half
    for n in range(0, half, step):
        at = pl.multiple_of(start + n, step)
        value = jnp.concatenate(
            [jnp.dot(a, b[:, pl.ds(at, step)], preferred_element_type=jnp.float32) for b in panels], 0
        )
        if coded:
            encode(value, out, slice(n, n + step))
        else:
            out[:, n : n + step] = value


def products(blocks, panels, half, coded):
    height = len(panels) * len(blocks) * blocks[0].shape[0]
    if coded:
        shape = jax.ShapeDtypeStruct((height + GROUPS * SUB, half), jnp.int16)
    else:
        shape = jax.ShapeDtypeStruct((height, half), jnp.float32)
    return pl.pallas_call(
        functools.partial(
            product_kernel, count=len(blocks), coded=coded, spread=panels[0].shape[1] // half
        ),
        out_shape=shape,
        in_specs=[VMEM] * (len(blocks) + len(panels)),
        out_specs=VMEM,
        compiler_params=SMALL,
        name="leaving" if coded else "staying",
    )(*blocks, *panels)


def coded_shape(height, half):
    return jax.ShapeDtypeStruct((height + GROUPS * SUB, half), jnp.int16)


def split_kernel(*refs, spread):
    codeds, kept, hold, send = refs[:-3], refs[-3], refs[-2], refs[-1]
    height = kept.shape[0] // 2
    each = kept.shape[0] // len(codeds)
    value = kept[...] + jnp.concatenate([decode(coded[...], each) for coded in codeds], 0)
    first, second = value[:height], value[height:]
    stays = places(spread)[1] == 0
    hold[...] = jnp.where(stays, first, second)
    encode(jnp.where(stays, second, first), send)


def split(codeds, kept, spread):
    height, half = kept.shape[0] // 2, kept.shape[1]
    return pl.pallas_call(
        functools.partial(split_kernel, spread=spread),
        out_shape=[jax.ShapeDtypeStruct((height, half), jnp.float32), coded_shape(height, half)],
        in_specs=[VMEM] * (len(codeds) + 1),
        out_specs=[VMEM, VMEM],
        compiler_params=SMALL,
        name="split",
    )(*codeds, kept)


def merge_kernel(*refs, count):
    codeds, kept, outs = refs[:count], refs[count], refs[count + 1 :]
    value = kept[...]
    for coded in codeds:
        value = value + decode(coded[...], kept.shape[0])
    for hold in outs[:-1]:
        hold[...] = value
    encode(value, outs[-1])


def merge(codeds, kept, holds):
    height, half = kept.shape
    out = pl.pallas_call(
        functools.partial(merge_kernel, count=len(codeds)),
        out_shape=[jax.ShapeDtypeStruct((height, half), jnp.float32)] * holds + [coded_shape(height, half)],
        in_specs=[VMEM] * (len(codeds) + 1),
        out_specs=[VMEM] * (holds + 1),
        compiler_params=SMALL,
        name="merge",
    )(*codeds, kept)
    return out if holds else (None, out[0])


def finish_kernel(*refs, count, heights, spread):
    kepts, codeds = refs[:count], refs[count : 2 * count]
    parts, out = refs[2 * count : -1], refs[-1]
    pick = places(spread)[2]
    value = jnp.concatenate(
        [kept[...] + decode(coded[...], kept.shape[0]) for kept, coded in zip(kepts, codeds)], 0
    )
    chunks = len(heights)
    for k in range(len(parts) // (2 * chunks)):
        pieces = []
        for j, height in enumerate(heights):
            at = 2 * (k * chunks + j)
            pieces.append(decode(parts[at][...], height) + decode(parts[at + 1][...], height))
        value = jnp.where(pick == k + 1, jnp.concatenate(pieces, 0), value)
    out[...] = value.astype(jnp.bfloat16)


def finish(kepts, codeds, parts, heights, spread):
    return pl.pallas_call(
        functools.partial(finish_kernel, count=len(kepts), heights=heights, spread=spread),
        out_shape=jax.ShapeDtypeStruct((sum(heights), kepts[0].shape[1]), jnp.bfloat16),
        in_specs=[VMEM] * (2 * len(kepts) + len(parts)),
        out_specs=VMEM,
        compiler_params=SMALL,
        name="finish",
    )(*kepts, *codeds, *parts)


def chosen_kernel(block, *refs, coded, spread):
    panels, out = refs[:-1], refs[-1]
    width = out.shape[1]
    step = min(width, 256)
    stays = places(spread)[1]
    for k, panel in enumerate(panels):

        @pl.when(stays == (1 - k if coded else k))
        def _():
            for n in range(0, width, step):
                at = slice(n, n + step)
                value = jnp.dot(block[...], panel[:, at], preferred_element_type=jnp.float32)
                if coded:
                    encode(value, out, at)
                else:
                    out[:, at] = value


def chosen(block, panels, spread, coded):
    height, width = block.shape[0], panels[0].shape[1]
    return pl.pallas_call(
        functools.partial(chosen_kernel, coded=coded, spread=spread),
        out_shape=coded_shape(height, width) if coded else jax.ShapeDtypeStruct((height, width), jnp.float32),
        in_specs=[VMEM] * 3,
        out_specs=VMEM,
        compiler_params=SMALL,
        name="chosen",
    )(block, *panels)


def quarter_kernel(block, first, second, *outs, coded, spread):
    half = outs[0].shape[1]
    step = min(half, 256)
    side, stays, _ = places(spread)
    here, there = side * half, (1 - side) * half

    def write(panel, start, out):
        for n in range(0, half, step):
            at = pl.ds(pl.multiple_of(start + n, step), step)
            value = jnp.dot(block[...], panel[:, at], preferred_element_type=jnp.float32)
            if coded:
                encode(value, out, slice(n, n + step))
            else:
                out[:, n : n + step] = value

    for k, (kept, left) in enumerate(((first, second), (second, first))):

        @pl.when(stays == k)
        def _():
            if coded:
                write(kept, there, outs[0])
                write(left, here, outs[1])
                write(left, there, outs[2])
            else:
                write(kept, here, outs[0])


def quarters(block, panels, spread, coded):
    height, half = block.shape[0], panels[0].shape[1] // spread
    kept = [jax.ShapeDtypeStruct((height, half), jnp.float32)]
    out = pl.pallas_call(
        functools.partial(quarter_kernel, coded=coded, spread=spread),
        out_shape=[coded_shape(height, half)] * 3 if coded else kept,
        in_specs=[VMEM] * 3,
        out_specs=[VMEM] * (3 if coded else 1),
        compiler_params=SMALL,
        name="quarters",
    )(block, *panels)
    return out if coded else out[0]


def halve_kernel(coded, kept, hold, send, *, spread):
    height, half = hold.shape
    side = places(spread)[0]

    def value(which):
        at = pl.ds(pl.multiple_of(which * half, half), half)
        return kept[:, at] + decode(coded[:, at], height)

    encode(value(1 - side), send)
    hold[...] = value(side)


def halve(coded, kept, spread):
    height, half = kept.shape[0], kept.shape[1] // spread
    return pl.pallas_call(
        functools.partial(halve_kernel, spread=spread),
        out_shape=[jax.ShapeDtypeStruct((height, half), jnp.float32), coded_shape(height, half)],
        in_specs=[VMEM, VMEM],
        out_specs=[VMEM, VMEM],
        compiler_params=SMALL,
        name="halve",
    )(coded, kept)


def after(value, *others):
    return lax.optimization_barrier((value, *others))[0]


def solution(mesh):
    rows, cols = mesh.shape["row"], mesh.shape["col"]
    spread = rows // cols
    assert spread == 2 and rows & (rows - 1) == 0 and cols >= 4

    def permute(value, move):
        pairs = [
            (r * cols + c, to[0] * cols + to[1])
            for r in range(rows)
            for c in range(cols)
            if (to := move(r, c)) is not None
        ]
        return lax.ppermute(value, ("row", "col"), pairs)

    last = cols // 2

    last = cols // 2
    inner = last - 2

    def met(r, c, bits):
        return not ((r // spread) ^ c) & bits

    def across(value):
        return permute(value, lambda r, c: (r ^ 1, c))

    def along(value):
        return permute(value, lambda r, c: (r ^ spread, c))

    def diagonal(value):
        return permute(value, lambda r, c: (r ^ spread ^ 1, c))

    def folded(send, hold):
        bit = 2
        while bit < last:
            got = permute(
                send,
                lambda r, c: (r ^ (bit * spread), c) if met(r, c, bit - 2) and not met(r, c, bit) else None,
            )
            hold, send = merge([got], hold, 1)
            bit *= 2
        return hold, send

    def body(tile_values, tile_counts, tile_cols, panels):
        half = panels.shape[1] // spread
        other = near_memory(permute(panels, lambda r, c: (r, c ^ 1)))
        *own, panels = [near_memory(x) for x in build(tile_values, tile_counts, tile_cols, panels)]
        chunks = len(PARTS)
        own, dense = own[:-chunks], {0: own[-chunks:]}
        bit = last
        while bit > 1:
            for m in list(dense):
                blocks = []
                for j in range(chunks):
                    blocks.append(near_memory(permute(dense[m][j], lambda r, c: (r, c ^ bit))))
                dense[m ^ bit] = blocks
            bit //= 2
        moved = [m for m in sorted(dense) if m]

        both = [panels, other]
        block = {name: [value] for name, value in zip(OWN, own)}
        for j in range(chunks):
            block[f"{j}"] = [dense[m][j] for m in moved]
        done, order = {}, []

        def tied(value):
            return after(value, *order) if order else value

        def multiply(name, k, coded):
            value = tied(block[name][k])
            if FIRST[name] == "x":
                return products([value], both, half, coded)
            return (chosen if FIRST[name] == "z" else quarters)(value, both, spread, coded)

        def leave(name, k):
            return multiply(name, k, True)

        def stay(name, k):
            return multiply(name, k, False)

        def first(name, k):
            value = done["leave", name][k]
            if FIRST[name] == "xz":
                return [across(value[0]), along(value[1]), diagonal(value[2])]
            return (across if FIRST[name] == "x" else along)(value)

        def separate(name, k):
            got, kept = tied(done["first", name][k]), done["stay", name][k]
            return split([got], kept, spread) if FIRST[name] == "x" else halve(got, kept, spread)

        def second(name, k):
            return (along if FIRST[name] == "x" else across)(done["split", name][k][1])

        def code(name, k):
            if FIRST[name] == "xz":
                gots, hold = list(done["first", name][k]), done["stay", name][k]
            else:
                gots, hold = [done["second", name][k]], done["split", name][k][0]
            gots[0] = tied(gots[0])
            if inner or name in OWN:
                return folded(*reversed(merge(gots, hold, 1)))
            return merge(gots, hold, 0)

        def near(name, k):
            m, bits = moved[k], inner if name in TURN else inner | last
            return permute(
                done["code", name][k][1], lambda r, c: (r, c ^ m) if met(r, c, bits) else None
            )

        def far(name, k):
            shift = last * spread
            if name in OWN or name not in TURN:
                m = 0 if name in OWN else moved[k]
                return permute(
                    done["code", name][k][1],
                    lambda r, c: (r ^ shift, c ^ m) if met(r, c, inner) and not met(r, c, last) else None,
                )
            m = moved[k]
            return permute(
                done["near", name][k],
                lambda r, c: (r ^ shift, c) if met(r, c ^ m, inner) and not met(r, c ^ m, last) else None,
            )

        actions = dict(leave=leave, stay=stay, first=first, split=separate, second=second, code=code, near=near, far=far)
        for step in PLAN:
            kind, name = step.split("_")
            results = []
            for k in range(len(block.get(name, (0,)))):
                results.append(actions[kind](name, k))
                if kind in KERNELS:
                    value = results[-1]
                    order = [value[-1] if isinstance(value, (tuple, list)) else value]
            done[kind, name] = results

        parts = []
        for k in range(len(moved)):
            for j in range(chunks):
                parts += [done["near", f"{j}"][k], done["far", f"{j}"][k]]
        kepts = [done["code", name][0][0] for name in OWN]
        heights = tuple(value.shape[0] for value in dense[0])
        return finish(kepts, [done["far", name][0] for name in OWN], parts, heights, spread)

    return jax.shard_map(
        body,
        mesh=mesh,
        in_specs=(P("row", "col", None), P("row", "col"), P("row", "col"), P("row", "col")),
        out_specs=P("col", "row"),
        check_vma=False,
    )
```

```python
import functools

import jax
import jax.numpy as jnp
from jax import lax
from jax.experimental import pallas as pl
from jax.experimental.pallas import tpu as pltpu
from jax.sharding import PartitionSpec as P


GROUPS = 1
SUB = 8
TOP = 32767.0
STEPS = 128.0
VMEM = pl.BlockSpec(memory_space=pltpu.VMEM)
SMALL = pltpu.CompilerParams(vmem_limit_bytes=16 * 2**20)


def encode(value, ref, at=slice(None)):
    height, width = value.shape
    part = height // GROUPS
    for g in range(GROUPS):
        rows = value[g * part : (g + 1) * part].reshape(part // SUB, SUB, width)
        largest = jnp.max(jnp.abs(rows), axis=0)
        code = jnp.ceil(jnp.log2(jnp.maximum(largest, 1e-30)) * STEPS)
        factor = TOP / jnp.exp2(code / STEPS)
        whole = jnp.clip(jnp.round(rows * factor[None]), -TOP, TOP).astype(jnp.int32)
        ref[g * part : (g + 1) * part, at] = whole.reshape(part, width).astype(jnp.int16)
        whole = code.astype(jnp.int32)
        code_rows = whole if g == 0 else jnp.concatenate([code_rows, whole], 0)
    ref[height : height + GROUPS * SUB, at] = code_rows.astype(jnp.int16)


def decode(coded, height):
    width = coded.shape[1]
    part = height // GROUPS
    codes = coded[height : height + GROUPS * SUB].astype(jnp.int32).astype(jnp.float32)
    pieces = []
    for g in range(GROUPS):
        scale = jnp.exp2(codes[g * SUB : (g + 1) * SUB] / STEPS) * (1.0 / TOP)
        rows = coded[g * part : (g + 1) * part].astype(jnp.int32).astype(jnp.float32)
        pieces.append((rows.reshape(part // SUB, SUB, width) * scale[None]).reshape(part, width))
    return jnp.concatenate(pieces, 0)


def places(spread):
    r, c = lax.axis_index("row"), lax.axis_index("col")
    q = r // spread
    return r % spread, (q + c) % 2, (q // 2) ^ (c // 2)


def near_memory(value):
    return pltpu.with_memory_space_constraint(value, pltpu.VMEM)


def far_memory(value):
    return pltpu.with_memory_space_constraint(value, pltpu.HBM)


FIRST = {"a": "x", "b": "z", "0": "xz", "1": "xz"}
OWN = ("a", "b")
PARTS = (144, 112)
TURN = ("0",)
PLAN = (
    "leave_a",
    "first_a",
    "leave_b",
    "first_b",
    "stay_a",
    "stay_b",
    "leave_0",
    "first_0",
    "split_a",
    "second_a",
    "split_b",
    "second_b",
    "stay_0",
    "leave_1",
    "first_1",
    "stay_1",
    "code_0",
    "near_0",
    "code_own",
    "far_own",
    "far_0",
    "code_1",
    "near_1",
    "far_1",
)
KERNELS = ("leave", "stay", "split", "code")


def build_kernel(counts_in, columns_in, tiles_in, panels_in, *refs):
    outs, (panels, counts, columns, tiles, sems) = refs[:-5], refs[-5:]
    copies = [
        pltpu.make_async_copy(source, target, sems.at[k])
        for k, (source, target) in enumerate(
            ((counts_in, counts), (columns_in, columns), (tiles_in, tiles), (panels_in, panels))
        )
    ]
    for copy in copies:
        copy.start()
    for copy in copies[:-1]:
        copy.wait()
    tall, slots = counts.shape[0], tiles.shape[0]
    wide = slots // tall
    edge = tiles.shape[1]
    start = jnp.int32(0)
    for i in range(tall):
        count = counts[i]
        for j in range(wide):
            slot, found = jnp.int32(0), jnp.int32(0)
            for t in range(wide):
                at = jnp.minimum(start + t, slots - 1)
                hit = (t < count) & (columns[at] == j)
                slot = jnp.where(hit, at, slot)
                found = jnp.where(hit, 1, found)
            tile = tiles[slot].astype(jnp.float32) * found.astype(jnp.float32)
            tile = tile.T.astype(jnp.bfloat16)
            at = slice(i * edge, (i + 1) * edge)
            outs[j][:, at] = tile
            top = 0
            for out in outs[wide:]:
                low, high = max(top, j * edge), min(top + out.shape[0], (j + 1) * edge)
                if low < high:
                    out[low - top : high - top, at] = tile[low - j * edge : high - j * edge]
                top += out.shape[0]
        start = start + count
    copies[-1].wait()


def build(tile_values, tile_counts, tile_cols, panels):
    slots, edge, _ = tile_values.shape
    tall = tile_counts.shape[0]
    wide = slots // tall
    heights = [edge] * wide + [part * edge // 128 for part in PARTS]
    return pl.pallas_call(
        build_kernel,
        out_shape=[jax.ShapeDtypeStruct((height, tall * edge), jnp.bfloat16) for height in heights]
        + [jax.ShapeDtypeStruct(panels.shape, panels.dtype)],
        in_specs=[pl.BlockSpec(memory_space=pltpu.HBM)] * 4,
        out_specs=[VMEM] * (len(heights) + 1),
        scratch_shapes=[
            pltpu.SMEM((tall,), jnp.int32),
            pltpu.SMEM((slots,), jnp.int32),
            pltpu.VMEM(tile_values.shape, tile_values.dtype),
            pltpu.SemaphoreType.DMA((4,)),
        ],
        compiler_params=SMALL,
        name="build",
    )(far_memory(tile_counts[:, 0]), far_memory(tile_cols[:, 0]), far_memory(tile_values), far_memory(panels))


def product_kernel(*refs, count, coded, spread):
    blocks, panels, out = refs[:count], refs[count:-1], refs[-1]
    a = jnp.concatenate([b[...] for b in blocks], 0) if count > 1 else blocks[0][...]
    half = out.shape[1]
    step = min(half, 256)
    side = places(spread)[0]
    start = (1 - side if coded else side) * half
    for n in range(0, half, step):
        at = pl.multiple_of(start + n, step)
        value = jnp.concatenate(
            [jnp.dot(a, b[:, pl.ds(at, step)], preferred_element_type=jnp.float32) for b in panels], 0
        )
        if coded:
            encode(value, out, slice(n, n + step))
        else:
            out[:, n : n + step] = value


def products(blocks, panels, half, coded):
    height = len(panels) * len(blocks) * blocks[0].shape[0]
    if coded:
        shape = jax.ShapeDtypeStruct((height + GROUPS * SUB, half), jnp.int16)
    else:
        shape = jax.ShapeDtypeStruct((height, half), jnp.float32)
    return pl.pallas_call(
        functools.partial(
            product_kernel, count=len(blocks), coded=coded, spread=panels[0].shape[1] // half
        ),
        out_shape=shape,
        in_specs=[VMEM] * (len(blocks) + len(panels)),
        out_specs=VMEM,
        compiler_params=SMALL,
        name="leaving" if coded else "staying",
    )(*blocks, *panels)


def coded_shape(height, half):
    return jax.ShapeDtypeStruct((height + GROUPS * SUB, half), jnp.int16)


def split_kernel(*refs, spread):
    codeds, kept, hold, send = refs[:-3], refs[-3], refs[-2], refs[-1]
    height = kept.shape[0] // 2
    each = kept.shape[0] // len(codeds)
    value = kept[...] + jnp.concatenate([decode(coded[...], each) for coded in codeds], 0)
    first, second = value[:height], value[height:]
    stays = places(spread)[1] == 0
    hold[...] = jnp.where(stays, first, second)
    encode(jnp.where(stays, second, first), send)


def split(codeds, kept, spread):
    height, half = kept.shape[0] // 2, kept.shape[1]
    return pl.pallas_call(
        functools.partial(split_kernel, spread=spread),
        out_shape=[jax.ShapeDtypeStruct((height, half), jnp.float32), coded_shape(height, half)],
        in_specs=[VMEM] * (len(codeds) + 1),
        out_specs=[VMEM, VMEM],
        compiler_params=SMALL,
        name="split",
    )(*codeds, kept)


def merge_kernel(*refs, count):
    codeds, kept, outs = refs[:count], refs[count], refs[count + 1 :]
    value = kept[...]
    for coded in codeds:
        value = value + decode(coded[...], kept.shape[0])
    for hold in outs[:-1]:
        hold[...] = value
    encode(value, outs[-1])


def merge(codeds, kept, holds):
    height, half = kept.shape
    out = pl.pallas_call(
        functools.partial(merge_kernel, count=len(codeds)),
        out_shape=[jax.ShapeDtypeStruct((height, half), jnp.float32)] * holds + [coded_shape(height, half)],
        in_specs=[VMEM] * (len(codeds) + 1),
        out_specs=[VMEM] * (holds + 1),
        compiler_params=SMALL,
        name="merge",
    )(*codeds, kept)
    return out if holds else (None, out[0])


def finish_kernel(*refs, count, heights, spread):
    kepts, codeds = refs[:count], refs[count : 2 * count]
    parts, out = refs[2 * count : -1], refs[-1]
    pick = places(spread)[2]
    value = jnp.concatenate(
        [kept[...] + decode(coded[...], kept.shape[0]) for kept, coded in zip(kepts, codeds)], 0
    )
    chunks = len(heights)
    for k in range(len(parts) // (2 * chunks)):
        pieces = []
        for j, height in enumerate(heights):
            at = 2 * (k * chunks + j)
            pieces.append(decode(parts[at][...], height) + decode(parts[at + 1][...], height))
        value = jnp.where(pick == k + 1, jnp.concatenate(pieces, 0), value)
    out[...] = value.astype(jnp.bfloat16)


def finish(kepts, codeds, parts, heights, spread):
    return pl.pallas_call(
        functools.partial(finish_kernel, count=len(kepts), heights=heights, spread=spread),
        out_shape=jax.ShapeDtypeStruct((sum(heights), kepts[0].shape[1]), jnp.bfloat16),
        in_specs=[VMEM] * (2 * len(kepts) + len(parts)),
        out_specs=VMEM,
        compiler_params=SMALL,
        name="finish",
    )(*kepts, *codeds, *parts)


def chosen_kernel(block, *refs, coded, spread):
    panels, out = refs[:-1], refs[-1]
    width = out.shape[1]
    step = min(width, 256)
    stays = places(spread)[1]
    for k, panel in enumerate(panels):

        @pl.when(stays == (1 - k if coded else k))
        def _():
            for n in range(0, width, step):
                at = slice(n, n + step)
                value = jnp.dot(block[...], panel[:, at], preferred_element_type=jnp.float32)
                if coded:
                    encode(value, out, at)
                else:
                    out[:, at] = value


def chosen(block, panels, spread, coded):
    height, width = block.shape[0], panels[0].shape[1]
    return pl.pallas_call(
        functools.partial(chosen_kernel, coded=coded, spread=spread),
        out_shape=coded_shape(height, width) if coded else jax.ShapeDtypeStruct((height, width), jnp.float32),
        in_specs=[VMEM] * 3,
        out_specs=VMEM,
        compiler_params=SMALL,
        name="chosen",
    )(block, *panels)


def quarter_kernel(block, first, second, *outs, coded, spread):
    half = outs[0].shape[1]
    step = min(half, 256)
    side, stays, _ = places(spread)
    here, there = side * half, (1 - side) * half

    def write(panel, start, out):
        for n in range(0, half, step):
            at = pl.ds(pl.multiple_of(start + n, step), step)
            value = jnp.dot(block[...], panel[:, at], preferred_element_type=jnp.float32)
            if coded:
                encode(value, out, slice(n, n + step))
            else:
                out[:, n : n + step] = value

    for k, (kept, left) in enumerate(((first, second), (second, first))):

        @pl.when(stays == k)
        def _():
            if coded:
                write(kept, there, outs[0])
                write(left, here, outs[1])
                write(left, there, outs[2])
            else:
                write(kept, here, outs[0])


def quarters(block, panels, spread, coded):
    height, half = block.shape[0], panels[0].shape[1] // spread
    kept = [jax.ShapeDtypeStruct((height, half), jnp.float32)]
    out = pl.pallas_call(
        functools.partial(quarter_kernel, coded=coded, spread=spread),
        out_shape=[coded_shape(height, half)] * 3 if coded else kept,
        in_specs=[VMEM] * 3,
        out_specs=[VMEM] * (3 if coded else 1),
        compiler_params=SMALL,
        name="quarters",
    )(block, *panels)
    return out if coded else out[0]


def halve_kernel(coded, kept, hold, send, *, spread):
    height, half = hold.shape
    side = places(spread)[0]

    def value(which):
        at = pl.ds(pl.multiple_of(which * half, half), half)
        return kept[:, at] + decode(coded[:, at], height)

    encode(value(1 - side), send)
    hold[...] = value(side)


def halve(coded, kept, spread):
    height, half = kept.shape[0], kept.shape[1] // spread
    return pl.pallas_call(
        functools.partial(halve_kernel, spread=spread),
        out_shape=[jax.ShapeDtypeStruct((height, half), jnp.float32), coded_shape(height, half)],
        in_specs=[VMEM, VMEM],
        out_specs=[VMEM, VMEM],
        compiler_params=SMALL,
        name="halve",
    )(coded, kept)


def join_kernel(*refs):
    count = (len(refs) - 2) // 2
    value = jnp.concatenate(
        [kept[...] + decode(coded[...], kept.shape[0]) for coded, kept in zip(refs[:count], refs[count:-2])], 0
    )
    refs[-2][...] = value
    encode(value, refs[-1])


def join(codeds, kepts):
    height, half = sum(kept.shape[0] for kept in kepts), kepts[0].shape[1]
    return pl.pallas_call(
        join_kernel,
        out_shape=[jax.ShapeDtypeStruct((height, half), jnp.float32), coded_shape(height, half)],
        in_specs=[VMEM] * (2 * len(kepts)),
        out_specs=[VMEM, VMEM],
        compiler_params=SMALL,
        name="join",
    )(*codeds, *kepts)


def after(value, *others):
    return lax.optimization_barrier((value, *others))[0]


def solution(mesh):
    rows, cols = mesh.shape["row"], mesh.shape["col"]
    spread = rows // cols
    assert spread == 2 and rows & (rows - 1) == 0 and cols >= 4

    def permute(value, move):
        pairs = [
            (r * cols + c, to[0] * cols + to[1])
            for r in range(rows)
            for c in range(cols)
            if (to := move(r, c)) is not None
        ]
        return lax.ppermute(value, ("row", "col"), pairs)

    last = cols // 2

    last = cols // 2
    inner = last - 2

    def met(r, c, bits):
        return not ((r // spread) ^ c) & bits

    def across(value):
        return permute(value, lambda r, c: (r ^ 1, c))

    def along(value):
        return permute(value, lambda r, c: (r ^ spread, c))

    def diagonal(value):
        return permute(value, lambda r, c: (r ^ spread ^ 1, c))

    def folded(send, hold):
        bit = 2
        while bit < last:
            got = permute(
                send,
                lambda r, c: (r ^ (bit * spread), c) if met(r, c, bit - 2) and not met(r, c, bit) else None,
            )
            hold, send = merge([got], hold, 1)
            bit *= 2
        return hold, send

    def body(tile_values, tile_counts, tile_cols, panels):
        half = panels.shape[1] // spread
        other = near_memory(permute(panels, lambda r, c: (r, c ^ 1)))
        *own, panels = [near_memory(x) for x in build(tile_values, tile_counts, tile_cols, panels)]
        chunks = len(PARTS)
        own, dense = own[:-chunks], {0: own[-chunks:]}
        bit = last
        while bit > 1:
            for m in list(dense):
                blocks = []
                for j in range(chunks):
                    blocks.append(near_memory(permute(dense[m][j], lambda r, c: (r, c ^ bit))))
                dense[m ^ bit] = blocks
            bit //= 2
        moved = [m for m in sorted(dense) if m]

        both = [panels, other]
        block = {name: [value] for name, value in zip(OWN, own)}
        for j in range(chunks):
            block[f"{j}"] = [dense[m][j] for m in moved]
        done, order = {}, []

        def tied(value):
            return after(value, *order) if order else value

        def multiply(name, k, coded):
            value = tied(block[name][k])
            if FIRST[name] == "x":
                return products([value], both, half, coded)
            return (chosen if FIRST[name] == "z" else quarters)(value, both, spread, coded)

        def leave(name, k):
            return multiply(name, k, True)

        def stay(name, k):
            return multiply(name, k, False)

        def first(name, k):
            value = done["leave", name][k]
            if FIRST[name] == "xz":
                return [across(value[0]), along(value[1]), diagonal(value[2])]
            return (across if FIRST[name] == "x" else along)(value)

        def separate(name, k):
            got, kept = tied(done["first", name][k]), done["stay", name][k]
            return split([got], kept, spread) if FIRST[name] == "x" else halve(got, kept, spread)

        def second(name, k):
            return (along if FIRST[name] == "x" else across)(done["split", name][k][1])

        def code(name, k):
            if name == "own":
                gots = [done["second", n][0] for n in OWN]
                gots[0] = tied(gots[0])
                return folded(*reversed(join(gots, [done["split", n][0][0] for n in OWN])))
            if FIRST[name] == "xz":
                gots, hold = list(done["first", name][k]), done["stay", name][k]
            else:
                gots, hold = [done["second", name][k]], done["split", name][k][0]
            gots[0] = tied(gots[0])
            if inner:
                return folded(*reversed(merge(gots, hold, 1)))
            return merge(gots, hold, 0)

        def near(name, k):
            m, bits = moved[k], inner if name in TURN else inner | last
            return permute(
                done["code", name][k][1], lambda r, c: (r, c ^ m) if met(r, c, bits) else None
            )

        def far(name, k):
            shift = last * spread
            if name == "own" or name not in TURN:
                m = 0 if name == "own" else moved[k]
                return permute(
                    done["code", name][k][1],
                    lambda r, c: (r ^ shift, c ^ m) if met(r, c, inner) and not met(r, c, last) else None,
                )
            m = moved[k]
            return permute(
                done["near", name][k],
                lambda r, c: (r ^ shift, c) if met(r, c ^ m, inner) and not met(r, c ^ m, last) else None,
            )

        actions = dict(leave=leave, stay=stay, first=first, split=separate, second=second, code=code, near=near, far=far)
        for step in PLAN:
            kind, name = step.split("_")
            results = []
            for k in range(len(block.get(name, (0,)))):
                results.append(actions[kind](name, k))
                if kind in KERNELS:
                    value = results[-1]
                    order = [value[-1] if isinstance(value, (tuple, list)) else value]
            done[kind, name] = results

        parts = []
        for k in range(len(moved)):
            for j in range(chunks):
                parts += [done["near", f"{j}"][k], done["far", f"{j}"][k]]
        kept, arrived = done["code", "own"][0][0], done["far", "own"][0]
        heights = tuple(value.shape[0] for value in dense[0])
        return finish([kept], [arrived], parts, heights, spread)

    return jax.shard_map(
        body,
        mesh=mesh,
        in_specs=(P("row", "col", None), P("row", "col"), P("row", "col"), P("row", "col")),
        out_specs=P("col", "row"),
        check_vma=False,
    )
```
